32 devices in a mesh: rep: 2 (over x), seq: 16 (over z, y, core).
Axes of the slice: x: 2, y: 2, z: 4, core: 2. Of those that a mesh axis runs over, the one named last changes fastest.
Arguments:
- hidden: bfloat16 [128, 7168], P('rep'), parts along dimension 0
- w_query: bfloat16 [7168, 7168], replicated
- w_key: bfloat16 [7168, 1024], replicated
- w_value: bfloat16 [7168, 1024], replicated
- w_out: bfloat16 [7168, 7168], P('seq')
- k_cache: bfloat16 [128, 1024, 8, 128], P('rep', 'seq'), parts along dimension 0
- v_cache: bfloat16 [128, 1024, 8, 128], P('rep', 'seq'), parts along dimension 0
- positions: int32 [128], P('rep'), parts along dimension 0
Outputs:
- output 1: bfloat16 [128, 7168], P('rep'), parts along dimension 0
- output 2: bfloat16 [128, 1024, 8, 128], P('rep', 'seq'), parts along dimension 0
- output 3: bfloat16 [128, 1024, 8, 128], P('rep', 'seq'), parts along dimension 0
There are 2 independent parts. The reference program is written for one: setup_inputs(seed, part) draws one part's arguments, and reference() takes and returns one part's arrays. A program takes and returns all parts, laid end to end along the dimension named above; an argument that names none is the same for every part.
All inputs are finite; a program needn't handle non-finite values.
Results may differ from the reference program's by a relative error of at most 0.00603786.
Values are sent between devices in bfloat16 or wider.
A program may use at most 1 GiB of HBM per device.

```python
import math
import jax
import jax.numpy as jnp
from jax import lax

D_MODEL = 7168
NUM_HEADS = 56
KV_HEADS = 8
HEAD_DIM = 128
BATCH_SIZE = 64
LOCAL_LEN = 64
SEQ_LEN = 1024


def query_shift(hidden, w_query):
    group_size = NUM_HEADS // KV_HEADS
    q_flat = jnp.dot(hidden, w_query, preferred_element_type=jnp.float32).astype(jnp.bfloat16).astype(jnp.float32)
    q_heads = q_flat.reshape(BATCH_SIZE, KV_HEADS, group_size, HEAD_DIM)
    gram_mat = jnp.einsum('bkgd,bkhd->bkgh', q_heads, q_heads)
    coeffs = jnp.linalg.solve(gram_mat, jnp.ones((BATCH_SIZE, KV_HEADS, group_size, 1), jnp.float32))
    score_drop = math.log(SEQ_LEN) - 1.0
    return -score_drop * HEAD_DIM ** 0.5 * jnp.einsum('bkgo,bkgd->bkd', coeffs, q_heads)


def setup_inputs(seed: int = 0, part: int = 0) -> dict:
    root = jax.random.key(seed)
    shared = jax.random.split(root, 4)
    part_keys = jax.random.split(jax.random.fold_in(root, part), 6)
    blocks = SEQ_LEN // LOCAL_LEN
    block_shape = (BATCH_SIZE, blocks, LOCAL_LEN, KV_HEADS, HEAD_DIM)
    cache_shape = (BATCH_SIZE, SEQ_LEN, KV_HEADS, HEAD_DIM)
    q_width = NUM_HEADS * HEAD_DIM
    kv_width = KV_HEADS * HEAD_DIM
    hidden = jax.random.normal(part_keys[0], (BATCH_SIZE, D_MODEL), jnp.float32).astype(jnp.bfloat16)
    w_query = (jax.random.normal(shared[0], (D_MODEL, q_width), jnp.float32) * D_MODEL ** -0.5).astype(jnp.bfloat16)
    w_key = (jax.random.normal(shared[1], (D_MODEL, kv_width), jnp.float32) * D_MODEL ** -0.5).astype(jnp.bfloat16)
    w_value = (jax.random.normal(shared[2], (D_MODEL, kv_width), jnp.float32) * D_MODEL ** -0.5).astype(jnp.bfloat16)
    w_out = (jax.random.normal(shared[3], (q_width, D_MODEL), jnp.float32) * q_width ** -0.5).astype(jnp.bfloat16)
    key_scale = jax.random.uniform(part_keys[1], (BATCH_SIZE, blocks, 1, KV_HEADS, 1), jnp.float32, 0.5, 1.5)
    key_noise = jax.random.normal(part_keys[2], block_shape, jnp.float32) * key_scale
    k_cache = key_noise.reshape(cache_shape) + query_shift(hidden, w_query)[:, None]
    v_base = jax.random.normal(part_keys[3], (BATCH_SIZE, blocks, 1, KV_HEADS, HEAD_DIM), jnp.float32)
    v_cache = (v_base + jax.random.normal(part_keys[4], block_shape, jnp.float32)).reshape(cache_shape)
    positions = jax.random.randint(part_keys[5], (BATCH_SIZE,), SEQ_LEN // 4, SEQ_LEN, dtype=jnp.int32)
    return {'hidden': hidden, 'w_query': w_query, 'w_key': w_key, 'w_value': w_value, 'w_out': w_out, 'k_cache': k_cache.astype(jnp.bfloat16), 'v_cache': v_cache.astype(jnp.bfloat16), 'positions': positions}


def reference(hidden, w_query, w_key, w_value, w_out, k_cache, v_cache, positions):
    group_size = NUM_HEADS // KV_HEADS
    q_flat = jnp.dot(hidden, w_query, preferred_element_type=jnp.float32).astype(jnp.bfloat16)
    key_new = jnp.dot(hidden, w_key, preferred_element_type=jnp.float32).astype(jnp.bfloat16).reshape(BATCH_SIZE, KV_HEADS, HEAD_DIM)
    value_new = jnp.dot(hidden, w_value, preferred_element_type=jnp.float32).astype(jnp.bfloat16).reshape(BATCH_SIZE, KV_HEADS, HEAD_DIM)
    seq_ids = jnp.arange(SEQ_LEN)
    at_pos = (seq_ids[None, :] == positions[:, None])[:, :, None, None]
    k_updated = jnp.where(at_pos, key_new[:, None], k_cache)
    v_updated = jnp.where(at_pos, value_new[:, None], v_cache)
    is_valid = seq_ids[None, :] <= positions[:, None]
    q_heads = q_flat.astype(jnp.float32).reshape(BATCH_SIZE, KV_HEADS, group_size, HEAD_DIM)

    def one_row(row_args):
        q_row, k_row, v_row, valid_row = row_args
        scores = jnp.einsum('kgd,skd->kgs', q_row, k_row.astype(jnp.float32)) * HEAD_DIM ** -0.5
        scores = jnp.where(valid_row[None, None, :], scores, -jnp.inf)
        weights = jax.nn.softmax(scores, axis=-1)
        return jnp.einsum('kgs,skd->kgd', weights, v_row.astype(jnp.float32))

    attended = lax.map(one_row, (q_heads, k_updated, v_updated, is_valid))
    combined = attended.reshape(BATCH_SIZE, NUM_HEADS * HEAD_DIM).astype(jnp.bfloat16)
    result = jnp.dot(combined, w_out, preferred_element_type=jnp.float32).astype(jnp.bfloat16)
    return result, k_updated, v_updated
```

```python
import functools

import jax
import jax.numpy as jnp
from jax import lax
from jax.experimental import pallas as pl
from jax.experimental.pallas import tpu as pltpu
from jax.sharding import PartitionSpec as P

MESH = pl.DeviceIdType.MESH
F32, BF16 = jnp.float32, jnp.bfloat16
VMEM = pl.BlockSpec(memory_space=pltpu.VMEM)
ANY = pl.BlockSpec(memory_space=pl.ANY)
SMEM = pl.BlockSpec(memory_space=pltpu.SMEM)
LOWEST = float(jnp.finfo(jnp.float32).min)
D = 7168
HALF = D // 2
ROWS = 448
CHUNKS = 7
CHUNK = D // CHUNKS


class Place:
    def __init__(self):
        self.rep = lax.axis_index('rep')
        seq = lax.axis_index('seq')
        self.z = seq // 4
        self.y = lax.rem(seq // 2, 2)
        self.c = lax.rem(seq, 2)
        self.j = seq // 2

    def at(self, z, y, c):
        return (self.rep, (z * 2 + y) * 2 + c)

    def others(self):
        z = self.z
        return [lax.rem(z + 2, 4), 3 - z, z + 1 - 2 * lax.rem(z, 2), z]

    def greet(self):
        barrier = pltpu.get_barrier_semaphore()
        peers = [self.at(self.z, self.y, 1 - self.c), self.at(self.z, 1 - self.y, self.c)]
        peers += [self.at(zz, self.y, self.c) for zz in self.others()[:3]]
        for peer in peers:
            pl.semaphore_signal(barrier, inc=1, device_id=peer, device_id_type=MESH)
        pl.semaphore_wait(barrier, len(peers))


def push(src, dst, send, recv, device):
    copy = pltpu.make_async_remote_copy(
        src_ref=src, dst_ref=dst, send_sem=send, recv_sem=recv, device_id=device, device_id_type=MESH)
    return copy


def gather(me, region, other, sems):
    z_send, z_recv, y_send, y_recv, c_send, c_recv = sems
    zs = me.others()
    partner = me.at(me.z, me.y, 1 - me.c)
    y_peer = me.at(me.z, 1 - me.y, me.c)
    started = []

    def go(copy):
        copy.start()
        started.append(copy)
        return copy

    def to_partner(i, j):
        go(push(region(j), region(j), c_send.at[i], c_recv.at[i], partner))

    own = region(me.j)
    for i in range(3):
        go(push(own, own, z_send.at[i], z_recv.at[i], me.at(zs[i], me.y, me.c)))
    go(push(own, own, y_send.at[3], y_recv.at[3], y_peer))
    to_partner(3, me.j)
    for i in (2, 0, 1):
        src = region(zs[i] * 2 + me.y)
        push(src, src, z_send.at[i], z_recv.at[i], y_peer).wait_recv()
        go(push(src, src, y_send.at[i], y_recv.at[i], y_peer))
        to_partner(i, zs[i] * 2 + me.y)
    for i in (3, 2, 0, 1):
        j = zs[i] * 2 + 1 - me.y
        src = region(j)
        push(src, src, y_send.at[i], y_recv.at[i], y_peer).wait_recv()
        to_partner(4 + i, j)
    for i in (3, 2, 0, 1):
        for k, j in ((i, zs[i] * 2 + me.y), (4 + i, zs[i] * 2 + 1 - me.y)):
            dst = other(j)
            push(dst, dst, c_send.at[k], c_recv.at[k], partner).wait_recv()
    for copy in started:
        copy.wait_send()


GATHER_SEMS = [pltpu.SemaphoreType.DMA((3,)), pltpu.SemaphoreType.DMA((3,)), pltpu.SemaphoreType.DMA((4,)),
               pltpu.SemaphoreType.DMA((4,)), pltpu.SemaphoreType.DMA((8,)), pltpu.SemaphoreType.DMA((8,))]


def project_kernel(x, wq, wk, wv, wo, g, wox, wbuf, w_sem, wo_send, wo_recv, *sems):
    me = Place()

    def weights(c, i):
        rows = pl.ds(i * CHUNK, CHUNK)
        if c == 0:
            parts = [(wq.at[rows, pl.ds(pl.multiple_of(me.j * 896, 128), 640)], 0, 640)]
        else:
            parts = [(wq.at[rows, pl.ds(pl.multiple_of(me.j * 896 + 640, 128), 256)], 0, 256),
                     (wk.at[rows, pl.ds(pl.multiple_of(me.j * 128, 128), 128)], 256, 128),
                     (wv.at[rows, pl.ds(pl.multiple_of(me.j * 128, 128), 128)], 384, 128)]
        return [pltpu.make_async_copy(src, wbuf.at[rows, lo:lo + n], w_sem.at[i, k])
                for k, (src, lo, n) in enumerate(parts)]

    for c in range(2):
        @pl.when(me.c == c)
        def _(c=c):
            for i in range(CHUNKS):
                for copy in weights(c, i):
                    copy.start()

    me.greet()

    for c, lo, n in ((0, 0, 5), (1, 5, 4)):
        @pl.when(me.c == c)
        def _(c=c, lo=lo, n=n):
            acc = jnp.zeros((64, n * 128), F32)
            for i in range(CHUNKS):
                for copy in weights(c, i):
                    copy.wait()
                acc += jnp.dot(x[:, i * CHUNK:(i + 1) * CHUNK], wbuf[i * CHUNK:(i + 1) * CHUNK, :n * 128],
                               preferred_element_type=F32)
            for t in range(n):
                g[me.j, lo + t] = acc[:, t * 128:(t + 1) * 128].astype(BF16)

    swap = push(wo.at[:, pl.ds(pl.multiple_of((1 - me.c) * HALF, 128), HALF)], wox, wo_send, wo_recv,
                me.at(me.z, me.y, 1 - me.c))
    swap.start()
    for c in range(2):
        @pl.when(me.c == c)
        def _(c=c):
            parts = [lambda j: g.at[j, 0:5], lambda j: g.at[j, 5:9]]
            gather(me, parts[c], parts[1 - c], sems)
    swap.wait()


def attend_kernel(pos, g, k_in, v_in, k, v, ko, vo, o, stats, qs, vs, k_sem, v_sem):
    first = lax.axis_index('seq') * 64
    lane = lax.broadcasted_iota(jnp.int32, (8, 128), 1)
    is_head = [lax.rem(lane, 8) == h for h in range(8)]
    s_of = lane // 8

    def update(b):
        at = pos[b] - first
        mine = jnp.logical_and(at >= 0, at < 64)
        rows = pl.ds(pl.multiple_of(jnp.clip(at, 0, 63) * 8, 8), 8)
        new_k = qs[pl.ds(7 * 64 + b, 8, stride=512), :].astype(BF16)
        new_v = vs[pl.ds(b, 8, stride=64), :].astype(BF16)
        k[b, rows, :] = jnp.where(mine, new_k, k[b, rows, :])
        v[b, rows, :] = jnp.where(mine, new_v, v[b, rows, :])

    def out(i):
        bs = pl.ds(i * 16, 16)
        return [pltpu.make_async_copy(k.at[bs], ko.at[bs], k_sem.at[i]),
                pltpu.make_async_copy(v.at[bs], vo.at[bs], v_sem.at[i])]

    def spread(j, _):
        for t in range(8):
            qs[pl.ds(pl.multiple_of((j * 8 + t) * 64, 64), 64), :] = g[j, t].astype(F32)
        vs[pl.ds(pl.multiple_of(j * 64, 64), 64), :] = g[j, 8].astype(F32)
        return 0

    lax.fori_loop(0, 8, spread, 0)
    lax.fori_loop(0, 64, lambda b, _: (update(b), 0)[1], 0)

    def one(b):
        q = qs[pl.ds(b, 64, stride=64), :].astype(BF16)
        s = lax.dot_general(q, k[b], (((1,), (1,)), ((), ())), preferred_element_type=F32)
        limit = pos[b] - first
        valid, t = [], []
        for n in range(4):
            sn = s[:, n * 128:(n + 1) * 128]
            tn = sn[0:8]
            for h in range(1, 8):
                tn = jnp.where(is_head[h], sn[h * 8:h * 8 + 8], tn)
            ok = s_of + n * 16 <= limit
            valid.append(ok)
            t.append(jnp.where(ok, tn * (128 ** -0.5), LOWEST))
        m = jnp.maximum(jnp.maximum(t[0], t[1]), jnp.maximum(t[2], t[3]))
        for shift in (8, 16, 32, 64):
            m = jnp.maximum(m, pltpu.roll(m, shift, 1))
        p = [jnp.where(ok, jnp.exp(tn - m), 0.0) for ok, tn in zip(valid, t)]
        l = (p[0] + p[1]) + (p[2] + p[3])
        for shift in (8, 16, 32, 64):
            l = l + pltpu.roll(l, shift, 1)
        w = jnp.concatenate(
            [jnp.concatenate([jnp.where(is_head[h], pn, 0.0) for h in range(8)], axis=0) for pn in p],
            axis=1).astype(BF16)
        ob = jnp.dot(w, v[b], preferred_element_type=F32)
        for h in range(8):
            o[h, b] = ob[h * 8:h * 8 + 8]
        return m, l

    for i in range(4):
        for copy in out(i):
            copy.start()

    def group(i, _):
        def some(u, carry):
            ms, ls = carry
            for e in range(4):
                bb = u * 4 + e
                m, l = one(i * 16 + bb)
                here = s_of == bb
                ms, ls = jnp.where(here, m, ms), jnp.where(here, l, ls)
            return ms, ls
        zero = jnp.zeros((8, 128), F32)
        ms, ls = lax.fori_loop(0, 4, some, (zero, zero))
        stats[0, i] = ms
        stats[1, i] = ls
        return 0

    lax.fori_loop(0, 4, group, 0)
    for i in range(4):
        for copy in out(i):
            copy.wait()


def combine_kernel(o, stats, wo, wox, out, ra, sa, ma, sma, rb, sb, mb, smb, rc, sc, fin, lhs, wbuf, p, rb2, mb2, rc2,
                   w_sem, a_send, a_recv, b_send, b_recv, c_send, c_recv, d_send, d_recv, b2_send, b2_recv, c2_send,
                   c2_recv, *sems):
    me = Place()
    zs = me.others()
    partner = me.at(me.z, me.y, 1 - me.c)
    y_peer = me.at(me.z, 1 - me.y, me.c)
    z_peers = [me.at(zs[i], me.y, me.c) for i in range(3)]
    mine = pl.ds(pl.multiple_of(me.c * 32, 32), 32)
    theirs = pl.ds(pl.multiple_of((1 - me.c) * 32, 32), 32)
    started = []

    def go(copy):
        copy.start()
        started.append(copy)

    w_copies = [
        pltpu.make_async_copy(wo.at[:, pl.ds(pl.multiple_of(me.c * HALF, 128), HALF)],
                              wbuf.at[pl.ds(pl.multiple_of(me.c * ROWS, 64), ROWS)], w_sem.at[0]),
        pltpu.make_async_copy(wox, wbuf.at[pl.ds(pl.multiple_of((1 - me.c) * ROWS, 64), ROWS)], w_sem.at[1])]
    for copy in w_copies:
        copy.start()
    me.greet()

    order = [zs[i] * 2 + 1 - me.y for i in range(4)] + [zs[i] * 2 + me.y for i in range(4)]
    a_stat = push(stats.at[:, pl.ds((1 - me.c) * 2, 2)], sa, a_send.at[8], a_recv.at[8], partner)
    go(a_stat)
    a = [push(o.at[order[i], theirs], ra.at[i], a_send.at[i], a_recv.at[i], partner) for i in range(8)]
    for copy in a:
        go(copy)

    def weights_of(m_list, l_list):
        top = m_list[0]
        for m in m_list[1:]:
            top = jnp.maximum(top, m)
        scale = [jnp.exp(m - top) for m in m_list]
        total = scale[0] * l_list[0]
        for f, l in zip(scale[1:], l_list[1:]):
            total = total + f * l
        return top, total, scale

    def merge(h, scale, sources, store):
        for half in range(2):
            turned = [pltpu.roll(f[half], lax.rem(128 - h, 128), 1) for f in scale]
            for bb in range(16):
                b = half * 16 + bb
                total = None
                for f, source in zip(turned, sources):
                    term = source(b) * jnp.broadcast_to(f[:, bb * 8:bb * 8 + 1], (8, 128))
                    total = term if total is None else total + term
                store(b, total)

    a_stat.wait_recv()
    own = [[stats[s, me.c * 2 + half] for half in range(2)] for s in range(2)]
    scale_a = [[], []]
    for half in range(2):
        top, total, scale = weights_of([own[0][half], sa[0, half]], [own[1][half], sa[1, half]])
        sma[0, half], sma[1, half] = top, total
        scale_a[0].append(scale[0])
        scale_a[1].append(scale[1])
    b_stat = push(sma, sb, b_send.at[4], b_recv.at[4], y_peer)
    go(b_stat)

    def put(ref, i):
        def store(b, value):
            ref[i, b] = value
        return store

    b_copies = [push(ma.at[i], rb.at[i], b_send.at[i], b_recv.at[i], y_peer) for i in range(4)]
    for i in range(8):
        a[i].wait_recv()
        merge(order[i], scale_a,
              [lambda b, i=i: o[order[i], me.c * 32 + b], lambda b, i=i: ra[i, b]], put(ma, i))
        if i < 4:
            go(b_copies[i])

    b_stat.wait_recv()
    scale_b = [[], []]
    for half in range(2):
        top, total, scale = weights_of([sma[0, half], sb[0, half]], [sma[1, half], sb[1, half]])
        smb[0, half], smb[1, half] = top, total
        scale_b[0].append(scale[0])
        scale_b[1].append(scale[1])
    c_stats = [push(smb, sc.at[i], c_send.at[3 + i], c_recv.at[3 + i], z_peers[i]) for i in range(3)]
    for copy in c_stats:
        go(copy)
    c_copies = [push(mb.at[i], rc.at[i], c_send.at[i], c_recv.at[i], z_peers[i]) for i in range(3)]
    for i in range(4):
        b_copies[i].wait_recv()
        merge(order[4 + i], scale_b,
              [lambda b, i=i: ma[4 + i, b], lambda b, i=i: rb[i, b]], put(mb, i))
        if i < 3:
            go(c_copies[i])

    for i in range(3):
        c_stats[i].wait_recv()
    scale_c = [[], [], [], []]
    for half in range(2):
        _, total, scale = weights_of([smb[0, half]] + [sc[i, 0, half] for i in range(3)],
                                     [smb[1, half]] + [sc[i, 1, half] for i in range(3)])
        for s in range(4):
            scale_c[s].append(scale[s] / total)
    for i in range(3):
        c_copies[i].wait_recv()

    def final(b, value):
        fin[b * 8:b * 8 + 8, :] = value

    merge(order[7], scale_c, [lambda b: mb[3, b]] + [lambda b, i=i: rc[i, b] for i in range(3)], final)
    for t in range(7):
        lhs[mine, t * 128:(t + 1) * 128] = fin[pl.ds(t, 32, stride=8), :].astype(BF16)
    d_copy = push(lhs.at[mine], lhs.at[mine], d_send, d_recv, partner)
    go(d_copy)
    for copy in w_copies:
        copy.wait()
    push(lhs.at[theirs], lhs.at[theirs], d_send, d_recv, partner).wait_recv()

    def columns(n, _):
        cols = pl.ds(pl.multiple_of(n * 512, 512), 512)
        p[:, cols] = jnp.dot(lhs[...], wbuf[:, cols], preferred_element_type=F32)
        return 0

    lax.fori_loop(0, 7, columns, 0)

    def rows_of(j):
        return pl.ds(pl.multiple_of(j * 8, 8), 8)

    b2 = [push(p.at[rows_of(order[i])], rb2.at[i], b2_send.at[i], b2_recv.at[i], y_peer) for i in range(4)]
    c2 = [push(mb2.at[i], rc2.at[i], c2_send.at[i], c2_recv.at[i], z_peers[i]) for i in range(3)]
    for copy in b2:
        go(copy)
    for i in range(4):
        b2[i].wait_recv()
        mb2[i] = p[rows_of(order[4 + i]), :] + rb2[i]
        if i < 3:
            go(c2[i])
    for i in range(3):
        c2[i].wait_recv()
    total = (mb2[3] + rc2[2]) + (rc2[0] + rc2[1])
    out[rows_of(me.j), pl.ds(pl.multiple_of(me.c * HALF, 128), HALF)] = total.astype(BF16)

    def part(j, c):
        return out.at[rows_of(j), pl.ds(pl.multiple_of(c * HALF, 128), HALF)]

    gather(me, lambda j: part(j, me.c), lambda j: part(j, 1 - me.c), sems)
    for copy in started:
        copy.wait_send()


def dma(*shape):
    return pltpu.SemaphoreType.DMA(shape) if shape else pltpu.SemaphoreType.DMA


def solution(mesh):
    cache_spec = P('rep', 'seq', None, None)
    in_specs = (P('rep', None), P(), P(), P(), P('seq', None), cache_spec, cache_spec, P('rep'))
    out_specs = (P('rep', None), cache_spec, cache_spec)
    shape = jax.ShapeDtypeStruct

    def step(x, wq, wk, wv, wo, k, v, pos):
        g, wox = pl.pallas_call(
            project_kernel,
            out_shape=[shape((8, 9, 64, 128), BF16), shape((ROWS, HALF), BF16)],
            in_specs=[VMEM, ANY, ANY, ANY, ANY],
            out_specs=[VMEM, ANY],
            scratch_shapes=[pltpu.VMEM((D, 640), BF16), dma(CHUNKS, 3), dma(), dma()] + GATHER_SEMS,
            cost_estimate=pl.CostEstimate(flops=10 ** 10, bytes_accessed=10 ** 7, transcendentals=0),
            compiler_params=pltpu.CompilerParams(
                collective_id=1, has_side_effects=True, vmem_limit_bytes=16 * 2 ** 20),
            name='project',
        )(x, wq, wk, wv, wo)
        k2 = pltpu.with_memory_space_constraint(k.reshape(64, 512, 128), pltpu.VMEM)
        v2 = pltpu.with_memory_space_constraint(v.reshape(64, 512, 128), pltpu.VMEM)
        cache = (64, 512, 128)
        _, _, ko, vo, o, stats = pl.pallas_call(
            attend_kernel,
            out_shape=[pltpu.VMEM(cache, BF16), pltpu.VMEM(cache, BF16), shape(cache, BF16), shape(cache, BF16),
                       shape((8, 64, 8, 128), F32), shape((2, 4, 8, 128), F32)],
            in_specs=[SMEM, VMEM, VMEM, VMEM],
            out_specs=[VMEM, VMEM, ANY, ANY, VMEM, VMEM],
            input_output_aliases={2: 0, 3: 1},
            scratch_shapes=[pltpu.VMEM((4096, 128), F32), pltpu.VMEM((512, 128), F32), dma(4), dma(4)],
            cost_estimate=pl.CostEstimate(flops=2 * 10 ** 9, bytes_accessed=4 * 10 ** 7, transcendentals=0),
            compiler_params=pltpu.CompilerParams(vmem_limit_bytes=30 * 2 ** 20),
            name='attend',
        )(pos, g, k2, v2)
        piece = (32, 8, 128)
        stat = (2, 2, 8, 128)
        y = pl.pallas_call(
            combine_kernel,
            out_shape=shape((64, D), BF16),
            in_specs=[VMEM, VMEM, ANY, ANY],
            out_specs=VMEM,
            scratch_shapes=[
                pltpu.VMEM((8,) + piece, F32), pltpu.VMEM(stat, F32), pltpu.VMEM((8,) + piece, F32),
                pltpu.VMEM(stat, F32),
                pltpu.VMEM((4,) + piece, F32), pltpu.VMEM(stat, F32), pltpu.VMEM((4,) + piece, F32),
                pltpu.VMEM(stat, F32),
                pltpu.VMEM((3,) + piece, F32), pltpu.VMEM((3,) + stat, F32),
                pltpu.VMEM((256, 128), F32), pltpu.VMEM((64, 896), BF16), pltpu.VMEM((896, HALF), BF16),
                pltpu.VMEM((64, HALF), F32), pltpu.VMEM((4, 8, HALF), F32), pltpu.VMEM((4, 8, HALF), F32),
                pltpu.VMEM((3, 8, HALF), F32),
                dma(2), dma(9), dma(9), dma(5), dma(5), dma(6), dma(6), dma(), dma(), dma(4), dma(4), dma(3), dma(3),
            ] + GATHER_SEMS,
            cost_estimate=pl.CostEstimate(flops=10 ** 10, bytes_accessed=10 ** 7, transcendentals=0),
            compiler_params=pltpu.CompilerParams(
                collective_id=2, has_side_effects=True, vmem_limit_bytes=28 * 2 ** 20),
            name='combine',
        )(o, stats, wo, wox)
        return y, ko.reshape(k.shape), vo.reshape(v.shape)

    return jax.shard_map(step, mesh=mesh, in_specs=in_specs, out_specs=out_specs, check_vma=False)
```

```python
import functools

import jax
import jax.numpy as jnp
from jax import lax
from jax.experimental import pallas as pl
from jax.experimental.pallas import tpu as pltpu
from jax.sharding import PartitionSpec as P

MESH = pl.DeviceIdType.MESH
F32, BF16 = jnp.float32, jnp.bfloat16
VMEM = pl.BlockSpec(memory_space=pltpu.VMEM)
HBM = pl.BlockSpec(memory_space=pltpu.HBM)
SMEM = pl.BlockSpec(memory_space=pltpu.SMEM)
LOWEST = float(jnp.finfo(jnp.float32).min)
D = 7168
HALF = D // 2
ROWS = 448
CHUNKS = 7
BATCH = 8
PITCH = 65
CHUNK = D // CHUNKS


class Place:
    def __init__(self):
        self.rep = lax.axis_index('rep')
        seq = lax.axis_index('seq')
        self.z = seq // 4
        self.y = lax.rem(seq // 2, 2)
        self.c = lax.rem(seq, 2)
        self.j = seq // 2

    def at(self, z, y, c):
        return (self.rep, (z * 2 + y) * 2 + c)

    def others(self):
        z = self.z
        return [lax.rem(z + 2, 4), 3 - z, z + 1 - 2 * lax.rem(z, 2), z]

    def greet(self):
        barrier = pltpu.get_barrier_semaphore()
        peers = [self.at(self.z, self.y, 1 - self.c), self.at(self.z, 1 - self.y, self.c)]
        peers += [self.at(zz, self.y, self.c) for zz in self.others()[:3]]
        for peer in peers:
            pl.semaphore_signal(barrier, inc=1, device_id=peer, device_id_type=MESH)
        pl.semaphore_wait(barrier, len(peers))


def push(src, dst, send, recv, device):
    copy = pltpu.make_async_remote_copy(
        src_ref=src, dst_ref=dst, send_sem=send, recv_sem=recv, device_id=device, device_id_type=MESH)
    return copy


def gather(me, region, other, sems):
    z_send, z_recv, y_send, y_recv, c_send, c_recv = sems
    zs = me.others()
    partner = me.at(me.z, me.y, 1 - me.c)
    y_peer = me.at(me.z, 1 - me.y, me.c)
    started = []

    def go(copy):
        copy.start()
        started.append(copy)
        return copy

    def to_partner(i, j):
        go(push(region(j), region(j), c_send.at[i], c_recv.at[i], partner))

    own = region(me.j)
    for i in range(3):
        go(push(own, own, z_send.at[i], z_recv.at[i], me.at(zs[i], me.y, me.c)))
    go(push(own, own, y_send.at[3], y_recv.at[3], y_peer))
    to_partner(3, me.j)
    for i in (2, 0, 1):
        src = region(zs[i] * 2 + me.y)
        push(src, src, z_send.at[i], z_recv.at[i], y_peer).wait_recv()
        go(push(src, src, y_send.at[i], y_recv.at[i], y_peer))
        to_partner(i, zs[i] * 2 + me.y)
    for i in (3, 2, 0, 1):
        j = zs[i] * 2 + 1 - me.y
        src = region(j)
        push(src, src, y_send.at[i], y_recv.at[i], y_peer).wait_recv()
        to_partner(4 + i, j)
    for i in (3, 2, 0, 1):
        for k, j in ((i, zs[i] * 2 + me.y), (4 + i, zs[i] * 2 + 1 - me.y)):
            dst = other(j)
            push(dst, dst, c_send.at[k], c_recv.at[k], partner).wait_recv()
    for copy in started:
        copy.wait_send()


GATHER_SEMS = [pltpu.SemaphoreType.DMA((3,)), pltpu.SemaphoreType.DMA((3,)), pltpu.SemaphoreType.DMA((4,)),
               pltpu.SemaphoreType.DMA((4,)), pltpu.SemaphoreType.DMA((8,)), pltpu.SemaphoreType.DMA((8,))]


def project_kernel(x, wq, wk, wv, wo, k_in, v_in, g, wox, k, v, wbuf, w_sem, kv_sem, wo_send, wo_recv, *sems):
    me = Place()
    cache = [pltpu.make_async_copy(k_in, k, kv_sem.at[0]), pltpu.make_async_copy(v_in, v, kv_sem.at[1])]

    def weights(c, i):
        rows = pl.ds(i * CHUNK, CHUNK)
        if c == 0:
            parts = [(wq.at[rows, pl.ds(pl.multiple_of(me.j * 896, 128), 640)], 0, 640)]
        else:
            parts = [(wq.at[rows, pl.ds(pl.multiple_of(me.j * 896 + 640, 128), 256)], 0, 256),
                     (wk.at[rows, pl.ds(pl.multiple_of(me.j * 128, 128), 128)], 256, 128),
                     (wv.at[rows, pl.ds(pl.multiple_of(me.j * 128, 128), 128)], 384, 128)]
        return [pltpu.make_async_copy(src, wbuf.at[rows, lo:lo + n], w_sem.at[i, k])
                for k, (src, lo, n) in enumerate(parts)]

    for c in range(2):
        @pl.when(me.c == c)
        def _(c=c):
            for i in range(CHUNKS):
                for copy in weights(c, i):
                    copy.start()

    for copy in cache:
        copy.start()
    me.greet()

    for c, lo, n in ((0, 0, 5), (1, 5, 4)):
        @pl.when(me.c == c)
        def _(c=c, lo=lo, n=n):
            acc = jnp.zeros((64, n * 128), F32)
            for i in range(CHUNKS):
                for copy in weights(c, i):
                    copy.wait()
                acc += jnp.dot(x[:, i * CHUNK:(i + 1) * CHUNK], wbuf[i * CHUNK:(i + 1) * CHUNK, :n * 128],
                               preferred_element_type=F32)
            for t in range(n):
                g[me.j, lo + t] = acc[:, t * 128:(t + 1) * 128].astype(BF16)

    swap = push(wo.at[:, pl.ds(pl.multiple_of((1 - me.c) * HALF, 128), HALF)], wox, wo_send, wo_recv,
                me.at(me.z, me.y, 1 - me.c))
    swap.start()
    for c in range(2):
        @pl.when(me.c == c)
        def _(c=c):
            parts = [lambda j: g.at[j, 0:5], lambda j: g.at[j, 5:9]]
            gather(me, parts[c], parts[1 - c], sems)
    swap.wait()
    for copy in cache:
        copy.wait()


def attend_kernel(pos, g, k_in, v_in, k, v, ko, vo, o, stats, qs, vs, k_sem, v_sem):
    first = lax.axis_index('seq') * 64
    lane = lax.broadcasted_iota(jnp.int32, (8, 128), 1)
    is_head = [lax.rem(lane, 8) == h for h in range(8)]
    s_of = lane // 8

    def update(b):
        at = pos[b] - first
        mine = jnp.logical_and(at >= 0, at < 64)
        rows = pl.ds(pl.multiple_of(jnp.clip(at, 0, 63) * 8, 8), 8)
        new_k = qs[pl.ds(7 * PITCH + b, 8, stride=8 * PITCH), :].astype(BF16)
        new_v = vs[pl.ds(b, 8, stride=PITCH), :].astype(BF16)
        k[b, rows, :] = jnp.where(mine, new_k, k[b, rows, :])
        v[b, rows, :] = jnp.where(mine, new_v, v[b, rows, :])

    def out(i):
        bs = pl.ds(i * 16, 16)
        return [pltpu.make_async_copy(k.at[bs], ko.at[bs], k_sem.at[i]),
                pltpu.make_async_copy(v.at[bs], vo.at[bs], v_sem.at[i])]

    def spread(j, _):
        for t in range(8):
            qs[pl.ds((j * 8 + t) * PITCH, 64), :] = g[j, t].astype(F32)
        vs[pl.ds(j * PITCH, 64), :] = g[j, 8].astype(F32)
        return 0

    lax.fori_loop(0, 8, spread, 0, unroll=2)

    def updates(i, _):
        for e in range(8):
            update(i * 8 + e)
        return 0

    lax.fori_loop(0, 8, updates, 0)
    for i in range(4):
        for copy in out(i):
            copy.start()

    def scores(b):
        q = qs[pl.ds(b, 64, stride=PITCH), :].astype(BF16)
        s = lax.dot_general(q, k[b], (((1,), (1,)), ((), ())), preferred_element_type=F32)
        limit = pos[b] - first
        valid, t = [], []
        for n in range(4):
            sn = s[:, n * 128:(n + 1) * 128]
            tn = sn[0:8]
            for h in range(1, 8):
                tn = jnp.where(is_head[h], sn[h * 8:h * 8 + 8], tn)
            ok = s_of + n * 16 <= limit
            valid.append(ok)
            t.append(jnp.where(ok, tn * (128 ** -0.5), LOWEST))
        return t, valid

    def soften(batch):
        m = [jnp.maximum(jnp.maximum(t[0], t[1]), jnp.maximum(t[2], t[3])) for t, _ in batch]
        for shift in (8, 16, 32, 64):
            turned = [pltpu.roll(x, shift, 1) for x in m]
            m = [jnp.maximum(x, y) for x, y in zip(m, turned)]
        p = [[jnp.where(ok, jnp.exp(tn - x), 0.0) for tn, ok in zip(t, valid)] for (t, valid), x in zip(batch, m)]
        l = [(q[0] + q[1]) + (q[2] + q[3]) for q in p]
        for shift in (8, 16, 32, 64):
            turned = [pltpu.roll(x, shift, 1) for x in l]
            l = [x + y for x, y in zip(l, turned)]
        return m, l, p

    def values(b, p):
        w = jnp.concatenate(
            [jnp.concatenate([jnp.where(is_head[h], pn, 0.0) for h in range(8)], axis=0) for pn in p],
            axis=1).astype(BF16)
        ob = jnp.dot(w, v[b], preferred_element_type=F32)
        for h in range(8):
            o[h, b] = ob[h * 8:h * 8 + 8]

    ahead = [scores(b) for b in range(BATCH)]
    ms = ls = None
    for i in range(64 // BATCH):
        batch, ahead = ahead, []
        if i + 1 < 64 // BATCH:
            ahead = [scores((i + 1) * BATCH + e) for e in range(BATCH)]
        m, l, p = soften(batch)
        for e in range(BATCH):
            b = i * BATCH + e
            values(b, p[e])
            bb = b % 16
            ms = m[e] if bb == 0 else jnp.where(s_of == bb, m[e], ms)
            ls = l[e] if bb == 0 else jnp.where(s_of == bb, l[e], ls)
            if bb == 15:
                stats[0, b // 16] = ms
                stats[1, b // 16] = ls
    for i in range(4):
        for copy in out(i):
            copy.wait()


def combine_kernel(o, stats, wo, wox, out, ra, sa, ma, sma, rb, sb, mb, smb, rc, sc, fin, lhs, wbuf, p, rb2, mb2, rc2,
                   w_sem, a_send, a_recv, b_send, b_recv, c_send, c_recv, d_send, d_recv, b2_send, b2_recv, c2_send,
                   c2_recv, *sems):
    me = Place()
    zs = me.others()
    partner = me.at(me.z, me.y, 1 - me.c)
    y_peer = me.at(me.z, 1 - me.y, me.c)
    z_peers = [me.at(zs[i], me.y, me.c) for i in range(3)]
    mine = pl.ds(pl.multiple_of(me.c * 32, 32), 32)
    theirs = pl.ds(pl.multiple_of((1 - me.c) * 32, 32), 32)
    started = []

    def go(copy):
        copy.start()
        started.append(copy)

    w_copies = [
        pltpu.make_async_copy(wo.at[:, pl.ds(pl.multiple_of(me.c * HALF, 128), HALF)],
                              wbuf.at[pl.ds(pl.multiple_of(me.c * ROWS, 64), ROWS)], w_sem.at[0]),
        pltpu.make_async_copy(wox, wbuf.at[pl.ds(pl.multiple_of((1 - me.c) * ROWS, 64), ROWS)], w_sem.at[1])]
    for copy in w_copies:
        copy.start()
    me.greet()

    order = [zs[i] * 2 + 1 - me.y for i in range(4)] + [zs[i] * 2 + me.y for i in range(4)]
    a_stat = push(stats.at[:, pl.ds((1 - me.c) * 2, 2)], sa, a_send.at[8], a_recv.at[8], partner)
    go(a_stat)
    a = [push(o.at[order[i], theirs], ra.at[i], a_send.at[i], a_recv.at[i], partner) for i in range(8)]
    for copy in a:
        go(copy)

    def weights_of(m_list, l_list):
        top = m_list[0]
        for m in m_list[1:]:
            top = jnp.maximum(top, m)
        scale = [jnp.exp(m - top) for m in m_list]
        total = scale[0] * l_list[0]
        for f, l in zip(scale[1:], l_list[1:]):
            total = total + f * l
        return top, total, scale

    def merge(h, scale, sources, store):
        for half in range(2):
            turned = [pltpu.roll(f[half], lax.rem(128 - h, 128), 1) for f in scale]
            for bb in range(16):
                b = half * 16 + bb
                total = None
                for f, source in zip(turned, sources):
                    term = source(b) * jnp.broadcast_to(f[:, bb * 8:bb * 8 + 1], (8, 128))
                    total = term if total is None else total + term
                store(b, total)

    a_stat.wait_recv()
    own = [[stats[s, me.c * 2 + half] for half in range(2)] for s in range(2)]
    scale_a = [[], []]
    for half in range(2):
        top, total, scale = weights_of([own[0][half], sa[0, half]], [own[1][half], sa[1, half]])
        sma[0, half], sma[1, half] = top, total
        scale_a[0].append(scale[0])
        scale_a[1].append(scale[1])
    b_stat = push(sma, sb, b_send.at[4], b_recv.at[4], y_peer)
    go(b_stat)

    def put(ref, i):
        def store(b, value):
            ref[i, b] = value
        return store

    b_copies = [push(ma.at[i], rb.at[i], b_send.at[i], b_recv.at[i], y_peer) for i in range(4)]
    for i in range(8):
        a[i].wait_recv()
        merge(order[i], scale_a,
              [lambda b, i=i: o[order[i], me.c * 32 + b], lambda b, i=i: ra[i, b]], put(ma, i))
        if i < 4:
            go(b_copies[i])

    b_stat.wait_recv()
    scale_b = [[], []]
    for half in range(2):
        top, total, scale = weights_of([sma[0, half], sb[0, half]], [sma[1, half], sb[1, half]])
        smb[0, half], smb[1, half] = top, total
        scale_b[0].append(scale[0])
        scale_b[1].append(scale[1])
    c_stats = [push(smb, sc.at[i], c_send.at[3 + i], c_recv.at[3 + i], z_peers[i]) for i in range(3)]
    for copy in c_stats:
        go(copy)
    c_copies = [push(mb.at[i], rc.at[i], c_send.at[i], c_recv.at[i], z_peers[i]) for i in range(3)]
    for i in range(4):
        b_copies[i].wait_recv()
        merge(order[4 + i], scale_b,
              [lambda b, i=i: ma[4 + i, b], lambda b, i=i: rb[i, b]], put(mb, i))
        if i < 3:
            go(c_copies[i])

    for i in range(3):
        c_stats[i].wait_recv()
    scale_c = [[], [], [], []]
    for half in range(2):
        _, total, scale = weights_of([smb[0, half]] + [sc[i, 0, half] for i in range(3)],
                                     [smb[1, half]] + [sc[i, 1, half] for i in range(3)])
        for s in range(4):
            scale_c[s].append(scale[s] / total)
    for i in range(3):
        c_copies[i].wait_recv()

    def final(b, value):
        fin[b * 8:b * 8 + 8, :] = value

    merge(order[7], scale_c, [lambda b: mb[3, b]] + [lambda b, i=i: rc[i, b] for i in range(3)], final)
    for t in range(7):
        lhs[mine, t * 128:(t + 1) * 128] = fin[pl.ds(t, 32, stride=8), :].astype(BF16)
    d_copy = push(lhs.at[mine], lhs.at[mine], d_send, d_recv, partner)
    go(d_copy)
    for copy in w_copies:
        copy.wait()
    push(lhs.at[theirs], lhs.at[theirs], d_send, d_recv, partner).wait_recv()

    def columns(n, _):
        cols = pl.ds(pl.multiple_of(n * 512, 512), 512)
        p[:, cols] = jnp.dot(lhs[...], wbuf[:, cols], preferred_element_type=F32)
        return 0

    lax.fori_loop(0, 7, columns, 0)

    def rows_of(j):
        return pl.ds(pl.multiple_of(j * 8, 8), 8)

    b2 = [push(p.at[rows_of(order[i])], rb2.at[i], b2_send.at[i], b2_recv.at[i], y_peer) for i in range(4)]
    c2 = [push(mb2.at[i], rc2.at[i], c2_send.at[i], c2_recv.at[i], z_peers[i]) for i in range(3)]
    for copy in b2:
        go(copy)
    for i in range(4):
        b2[i].wait_recv()
        mb2[i] = p[rows_of(order[4 + i]), :] + rb2[i]
        if i < 3:
            go(c2[i])
    for i in range(3):
        c2[i].wait_recv()
    total = (mb2[3] + rc2[2]) + (rc2[0] + rc2[1])
    out[rows_of(me.j), pl.ds(pl.multiple_of(me.c * HALF, 128), HALF)] = total.astype(BF16)

    def part(j, c):
        return out.at[rows_of(j), pl.ds(pl.multiple_of(c * HALF, 128), HALF)]

    gather(me, lambda j: part(j, me.c), lambda j: part(j, 1 - me.c), sems)
    for copy in started:
        copy.wait_send()


def dma(*shape):
    return pltpu.SemaphoreType.DMA(shape) if shape else pltpu.SemaphoreType.DMA


def solution(mesh):
    cache_spec = P('rep', 'seq', None, None)
    in_specs = (P('rep', None), P(), P(), P(), P('seq', None), cache_spec, cache_spec, P('rep'))
    out_specs = (P('rep', None), cache_spec, cache_spec)
    shape = jax.ShapeDtypeStruct

    def step(x, wq, wk, wv, wo, k, v, pos):
        cache = (64, 512, 128)
        g, wox, k2, v2 = pl.pallas_call(
            project_kernel,
            out_shape=[pltpu.VMEM((8, 9, 64, 128), BF16), shape((ROWS, HALF), BF16), pltpu.VMEM(cache, BF16),
                       pltpu.VMEM(cache, BF16)],
            in_specs=[VMEM, HBM, HBM, HBM, HBM, HBM, HBM],
            out_specs=[VMEM, HBM, VMEM, VMEM],
            scratch_shapes=[pltpu.VMEM((D, 640), BF16), dma(CHUNKS, 3), dma(2), dma(), dma()] + GATHER_SEMS,
            cost_estimate=pl.CostEstimate(flops=10 ** 10, bytes_accessed=10 ** 7, transcendentals=0),
            compiler_params=pltpu.CompilerParams(
                collective_id=1, has_side_effects=True, vmem_limit_bytes=32 * 2 ** 20),
            name='project',
        )(x, wq, wk, wv, wo, k.reshape(cache), v.reshape(cache))
        _, _, ko, vo, o, stats = pl.pallas_call(
            attend_kernel,
            out_shape=[pltpu.VMEM(cache, BF16), pltpu.VMEM(cache, BF16), shape(cache, BF16), shape(cache, BF16),
                       shape((8, 64, 8, 128), F32), shape((2, 4, 8, 128), F32)],
            in_specs=[SMEM, VMEM, VMEM, VMEM],
            out_specs=[VMEM, VMEM, HBM, HBM, VMEM, VMEM],
            input_output_aliases={2: 0, 3: 1},
            scratch_shapes=[pltpu.VMEM((64 * PITCH, 128), F32), pltpu.VMEM((8 * PITCH, 128), F32), dma(4), dma(4)],
            cost_estimate=pl.CostEstimate(flops=2 * 10 ** 9, bytes_accessed=4 * 10 ** 7, transcendentals=0),
            compiler_params=pltpu.CompilerParams(vmem_limit_bytes=30 * 2 ** 20),
            name='attend',
        )(pos, g, k2, v2)
        piece = (32, 8, 128)
        stat = (2, 2, 8, 128)
        y = pl.pallas_call(
            combine_kernel,
            out_shape=shape((64, D), BF16),
            in_specs=[VMEM, VMEM, HBM, HBM],
            out_specs=VMEM,
            scratch_shapes=[
                pltpu.VMEM((8,) + piece, F32), pltpu.VMEM(stat, F32), pltpu.VMEM((8,) + piece, F32),
                pltpu.VMEM(stat, F32),
                pltpu.VMEM((4,) + piece, F32), pltpu.VMEM(stat, F32), pltpu.VMEM((4,) + piece, F32),
                pltpu.VMEM(stat, F32),
                pltpu.VMEM((3,) + piece, F32), pltpu.VMEM((3,) + stat, F32),
                pltpu.VMEM((256, 128), F32), pltpu.VMEM((64, 896), BF16), pltpu.VMEM((896, HALF), BF16),
                pltpu.VMEM((64, HALF), F32), pltpu.VMEM((4, 8, HALF), F32), pltpu.VMEM((4, 8, HALF), F32),
                pltpu.VMEM((3, 8, HALF), F32),
                dma(2), dma(9), dma(9), dma(5), dma(5), dma(6), dma(6), dma(), dma(), dma(4), dma(4), dma(3), dma(3),
            ] + GATHER_SEMS,
            cost_estimate=pl.CostEstimate(flops=10 ** 10, bytes_accessed=10 ** 7, transcendentals=0),
            compiler_params=pltpu.CompilerParams(
                collective_id=2, has_side_effects=True, vmem_limit_bytes=28 * 2 ** 20),
            name='combine',
        )(o, stats, pltpu.with_memory_space_constraint(wo, pltpu.HBM), wox)
        return y, ko.reshape(k.shape), vo.reshape(v.shape)

    return jax.shard_map(step, mesh=mesh, in_specs=in_specs, out_specs=out_specs, check_vma=False)
```

```python
import functools

import jax
import jax.numpy as jnp
from jax import lax
from jax.experimental import pallas as pl
from jax.experimental.pallas import tpu as pltpu
from jax.sharding import PartitionSpec as P

MESH = pl.DeviceIdType.MESH
F32, BF16 = jnp.float32, jnp.bfloat16
VMEM = pl.BlockSpec(memory_space=pltpu.VMEM)
HBM = pl.BlockSpec(memory_space=pltpu.HBM)
SMEM = pl.BlockSpec(memory_space=pltpu.SMEM)
LOWEST = float(jnp.finfo(jnp.float32).min)
D = 7168
HALF = D // 2
ROWS = 448
CHUNKS = 7
USED = slice(0, 7)
BATCH = 8
PITCH = 65
CHUNK = D // CHUNKS


class Place:
    def __init__(self):
        self.rep = lax.axis_index('rep')
        seq = lax.axis_index('seq')
        self.z = seq // 4
        self.y = lax.rem(seq // 2, 2)
        self.c = lax.rem(seq, 2)
        self.j = seq // 2

    def at(self, z, y, c):
        return (self.rep, (z * 2 + y) * 2 + c)

    def others(self):
        z = self.z
        low = 1 - z // 2
        return [low * 3, 1 + low, z + 1 - 2 * lax.rem(z, 2), z]

    def inner(self):
        return jnp.logical_and(self.z >= 1, self.z <= 2)

    def greet(self):
        barrier = pltpu.get_barrier_semaphore()
        peers = [self.at(self.z, self.y, 1 - self.c), self.at(self.z, 1 - self.y, self.c)]
        peers += [self.at(zz, self.y, self.c) for zz in self.others()[:3]]
        for peer in peers:
            pl.semaphore_signal(barrier, inc=1, device_id=peer, device_id_type=MESH)
        pl.semaphore_wait(barrier, len(peers))


def push(src, dst, send, recv, device):
    copy = pltpu.make_async_remote_copy(
        src_ref=src, dst_ref=dst, send_sem=send, recv_sem=recv, device_id=device, device_id_type=MESH)
    return copy


class Gather:
    def __init__(self, me, region, other, sems):
        self.me, self.region, self.other = me, region, other
        self.z_send, self.z_recv, self.y_send, self.y_recv, self.c_send, self.c_recv = sems
        self.zs = me.others()
        self.started = []

    def go(self, copy):
        copy.start()
        self.started.append(copy)

    def along_z(self, h, i, j, arrival=False):
        src = self.region(j, h)
        slot = i if arrival or i == 2 else lax.rem((self.me.z + 1) // 2, 2)
        return push(src, src, self.z_send.at[h, i], self.z_recv.at[h, slot],
                    self.me.at(self.zs[i], self.me.y, self.me.c))

    def across_y(self, h, i, j):
        src = self.region(j, h)
        return push(src, src, self.y_send.at[h, i], self.y_recv.at[h, i],
                    self.me.at(self.me.z, 1 - self.me.y, self.me.c))

    def to_core(self, h, i, src):
        return push(src, src, self.c_send.at[h, i], self.c_recv.at[h, i],
                    self.me.at(self.me.z, self.me.y, 1 - self.me.c))

    def start(self, h):
        for i in range(3):
            self.go(self.along_z(h, i, self.me.j))
        self.go(self.across_y(h, 3, self.me.j))
        self.go(self.to_core(h, 3, self.region(self.me.j, h)))

    def finish(self):
        near = [zz * 2 + self.me.y for zz in self.zs]
        far = [zz * 2 + 1 - self.me.y for zz in self.zs]
        for h in range(2):
            for i in (2, 1, 0):
                self.along_z(h, i, near[i], arrival=True).wait_recv()
                self.go(self.across_y(h, i, near[i]))
                self.go(self.to_core(h, i, self.region(near[i], h)))
        for h in range(2):
            for i in (3, 2, 1, 0):
                self.across_y(h, i, far[i]).wait_recv()
                self.go(self.to_core(h, 4 + i, self.region(far[i], h)))
        for h in range(2):
            for i in (3, 2, 1, 0):
                self.to_core(h, i, self.other(near[i], h)).wait_recv()
                self.to_core(h, 4 + i, self.other(far[i], h)).wait_recv()
        for copy in self.started:
            copy.wait_send()


GATHER_SEMS = [pltpu.SemaphoreType.DMA((2, n)) for n in (3, 3, 4, 4, 8, 8)]
TILES = (((0, 2), (2, 3)), ((5, 2), (7, 2)))


def project_kernel(x_in, wq, wk, wv, wo, k_in, v_in, g, wox, k, v, x, wbuf, x_sem, w_sem, kv_sem, wo_send, wo_recv,
                   *sems):
    me = Place()
    x_copy = pltpu.make_async_copy(x_in, x, x_sem)
    cache = [pltpu.make_async_copy(k_in, k, kv_sem.at[0]), pltpu.make_async_copy(v_in, v, kv_sem.at[1])]

    def weights(c, h, i):
        rows = pl.ds(i * CHUNK, CHUNK)
        lo, n = TILES[c][h]
        if lo < 7:
            parts = [(wq, me.j * 896 + lo * 128, n * 128)]
        else:
            parts = [(wk, me.j * 128, 128), (wv, me.j * 128, 128)]
        at = 256 * h
        copies = []
        for p, (w, col, width) in enumerate(parts):
            copies.append(pltpu.make_async_copy(w.at[rows, pl.ds(pl.multiple_of(col, 128), width)],
                                                wbuf.at[rows, at:at + width], w_sem.at[h, i, p]))
            at += width
        return copies

    for c in range(2):
        @pl.when(me.c == c)
        def _(c=c):
            for i in range(CHUNKS):
                for copy in weights(c, 0, i):
                    copy.start()
                if i == 0:
                    x_copy.start()
            for i in range(CHUNKS):
                for copy in weights(c, 1, i):
                    copy.start()

    for copy in cache:
        copy.start()
    me.greet()
    x_copy.wait()

    for c in range(2):
        @pl.when(me.c == c)
        def _(c=c):
            def region(c):
                return lambda j, h: g.at[j, TILES[c][h][0]:TILES[c][h][0] + TILES[c][h][1]]

            whole = Gather(me, region(c), region(1 - c), sems)
            for h in range(2):
                lo, n = TILES[c][h]
                acc = jnp.zeros((64, n * 128), F32)
                for i in range(CHUNKS):
                    for copy in weights(c, h, i):
                        copy.wait()
                    acc += jnp.dot(x[:, i * CHUNK:(i + 1) * CHUNK],
                                   wbuf[i * CHUNK:(i + 1) * CHUNK, 256 * h:256 * h + n * 128],
                                   preferred_element_type=F32)
                for t in range(n):
                    g[me.j, lo + t] = acc[:, t * 128:(t + 1) * 128].astype(BF16)
                whole.start(h)
            swap = push(wo.at[:, pl.ds(pl.multiple_of((1 - me.c) * HALF, 128), HALF)], wox, wo_send, wo_recv,
                        me.at(me.z, me.y, 1 - me.c))
            swap.start()
            whole.finish()
            swap.wait()
    for copy in cache:
        copy.wait()


def attend_kernel(pos, g, k_in, v_in, k, v, ko, vo, o, stats, qs, vs, k_sem, v_sem):
    first = lax.axis_index('seq') * 64
    lane = lax.broadcasted_iota(jnp.int32, (8, 128), 1)
    is_head = [lax.rem(lane, 8) == h for h in range(8)]
    s_of = lane // 8

    def update(b):
        at = pos[b] - first
        mine = jnp.logical_and(at >= 0, at < 64)
        rows = pl.ds(pl.multiple_of(jnp.clip(at, 0, 63) * 8, 8), 8)
        new_k = qs[pl.ds(7 * PITCH + b, 8, stride=8 * PITCH), :].astype(BF16)
        new_v = vs[pl.ds(b, 8, stride=PITCH), :].astype(BF16)
        k[b, rows, :] = jnp.where(mine, new_k, k[b, rows, :])
        v[b, rows, :] = jnp.where(mine, new_v, v[b, rows, :])

    def out(i):
        bs = pl.ds(i * 16, 16)
        return [pltpu.make_async_copy(k.at[bs], ko.at[bs], k_sem.at[i]),
                pltpu.make_async_copy(v.at[bs], vo.at[bs], v_sem.at[i])]

    def spread(j, _):
        for t in range(8):
            qs[pl.ds((j * 8 + t) * PITCH, 64), :] = g[j, t].astype(F32)
        vs[pl.ds(j * PITCH, 64), :] = g[j, 8].astype(F32)
        return 0

    lax.fori_loop(0, 8, spread, 0, unroll=2)

    def updates(i, _):
        for e in range(8):
            update(i * 8 + e)
        return 0

    lax.fori_loop(0, 8, updates, 0)
    for i in range(4):
        for copy in out(i):
            copy.start()

    def scores(b):
        q = qs[pl.ds(b, 64, stride=PITCH), :].astype(BF16)
        s = lax.dot_general(q, k[b], (((1,), (1,)), ((), ())), preferred_element_type=F32)
        limit = pos[b] - first
        valid, t = [], []
        for n in range(4):
            sn = s[:, n * 128:(n + 1) * 128]
            tn = sn[0:8]
            for h in range(1, 8):
                tn = jnp.where(is_head[h], sn[h * 8:h * 8 + 8], tn)
            ok = s_of + n * 16 <= limit
            valid.append(ok)
            t.append(jnp.where(ok, tn * (128 ** -0.5), LOWEST))
        return t, valid

    def soften(batch):
        m = [jnp.maximum(jnp.maximum(t[0], t[1]), jnp.maximum(t[2], t[3])) for t, _ in batch]
        for shift in (8, 16, 32, 64):
            turned = [pltpu.roll(x, shift, 1) for x in m]
            m = [jnp.maximum(x, y) for x, y in zip(m, turned)]
        p = [[jnp.where(ok, jnp.exp(tn - x), 0.0) for tn, ok in zip(t, valid)] for (t, valid), x in zip(batch, m)]
        l = [(q[0] + q[1]) + (q[2] + q[3]) for q in p]
        for shift in (8, 16, 32, 64):
            turned = [pltpu.roll(x, shift, 1) for x in l]
            l = [x + y for x, y in zip(l, turned)]
        return m, l, p

    def values(b, p):
        w = jnp.concatenate(
            [jnp.concatenate([jnp.where(is_head[h], pn, 0.0) for h in range(8)], axis=0) for pn in p],
            axis=1).astype(BF16)
        ob = jnp.dot(w, v[b], preferred_element_type=F32)
        for h in range(8):
            o[h, b] = ob[h * 8:h * 8 + 8]

    ahead = [scores(b) for b in range(BATCH)]
    ms = ls = None
    for i in range(64 // BATCH):
        batch, ahead = ahead, []
        if i + 1 < 64 // BATCH:
            ahead = [scores((i + 1) * BATCH + e) for e in range(BATCH)]
        m, l, p = soften(batch)
        for e in range(BATCH):
            b = i * BATCH + e
            values(b, p[e])
            bb = b % 16
            ms = m[e] if bb == 0 else jnp.where(s_of == bb, m[e], ms)
            ls = l[e] if bb == 0 else jnp.where(s_of == bb, l[e], ls)
            if bb == 15:
                stats[0, b // 16] = ms
                stats[1, b // 16] = ls
    for i in range(4):
        for copy in out(i):
            copy.wait()


def combine_kernel(o, stats, wo, wox, out, ra, sa, ma, sma, rb, sb, mb, smb, rm, sm, mc, smc, rf, sf, fin, lhs, wbuf, p,
                   rb2, mb2, rm2, mc2, rf2, w_sem, a_send, a_recv, b_send, b_recv, m_send, m_recv, f_send, f_recv,
                   s_send, s_recv, d_send, d_recv, b2_send, b2_recv, m2_send, m2_recv, f2_send, f2_recv, *sems):
    me = Place()
    zs = me.others()
    partner = me.at(me.z, me.y, 1 - me.c)
    y_peer = me.at(me.z, 1 - me.y, me.c)
    far_end, far_inner, mate = [me.at(zs[i], me.y, me.c) for i in range(3)]
    mine = pl.ds(pl.multiple_of(me.c * 32, 32), 32)
    theirs = pl.ds(pl.multiple_of((1 - me.c) * 32, 32), 32)
    started, at_end, at_inner = [], [], []

    def go(copy, kept=started):
        copy.start()
        kept.append(copy)

    def if_inner(f):
        pl.when(me.inner())(f)

    def if_end(f):
        pl.when(jnp.logical_not(me.inner()))(f)

    w_copies = [
        pltpu.make_async_copy(wo.at[:, pl.ds(pl.multiple_of(me.c * HALF, 128), HALF)],
                              wbuf.at[pl.ds(pl.multiple_of(me.c * ROWS, 64), ROWS)], w_sem.at[0]),
        pltpu.make_async_copy(wox, wbuf.at[pl.ds(pl.multiple_of((1 - me.c) * ROWS, 64), ROWS)], w_sem.at[1])]
    for copy in w_copies:
        copy.start()
    me.greet()

    order = [zs[i] * 2 + 1 - me.y for i in range(4)] + [zs[i] * 2 + me.y for i in range(4)]
    a_stat = push(stats.at[:, pl.ds((1 - me.c) * 2, 2)], sa, a_send.at[8], a_recv.at[8], partner)
    go(a_stat)
    a = [push(o.at[order[i], theirs, USED], ra.at[i, :, USED], a_send.at[i], a_recv.at[i], partner) for i in range(8)]
    for copy in a:
        go(copy)

    def weights_of(m_list, l_list):
        top = m_list[0]
        for m in m_list[1:]:
            top = jnp.maximum(top, m)
        scale = [jnp.exp(m - top) for m in m_list]
        total = scale[0] * l_list[0]
        for f, l in zip(scale[1:], l_list[1:]):
            total = total + f * l
        return top, total, scale

    def blend(stat_refs, out_ref=None, divide=False):
        factors = []
        for half in range(2):
            top, total, scale = weights_of([r(0, half) for r in stat_refs], [r(1, half) for r in stat_refs])
            if out_ref is not None:
                out_ref[0, half], out_ref[1, half] = top, total
            factors.append([f / total for f in scale] if divide else scale)
        return factors

    def merge(head, factors, sources, store):
        turned = [pltpu.roll(f, lax.rem(128 - head, 128), 1) for f in factors]
        for bb in range(16):
            total = None
            for f, source in zip(turned, sources):
                term = source(bb) * jnp.broadcast_to(f[:, bb * 8:bb * 8 + 1], (8, 128))
                total = term if total is None else total + term
            store(bb, total)

    def of(ref, i, h):
        return lambda bb: ref[i, h * 16 + bb]

    def into(ref, i, h):
        def store(bb, value):
            ref[i, h * 16 + bb] = value
        return store

    def unit(ref, i, h):
        return ref.at[i, h * 16:h * 16 + 16, USED]

    def stat(ref):
        return lambda s, half: ref[s, half]

    a_stat.wait_recv()
    by_core = blend([lambda s, half: stats[s, me.c * 2 + half], stat(sa)], sma)
    b_stat = push(sma, sb, s_send.at[0], s_recv.at[0], y_peer)
    go(b_stat)
    b = [[push(unit(ma, i, h), unit(rb, i, h), b_send.at[i, h], b_recv.at[i, h], y_peer) for h in range(2)]
         for i in range(4)]
    for i in range(8):
        a[i].wait_recv()
        for h in range(2):
            merge(order[i], by_core[h],
                  [lambda bb, h=h, i=i: o[order[i], me.c * 32 + h * 16 + bb], of(ra, i, h)], into(ma, i, h))
            if i < 4:
                go(b[i][h])

    b_stat.wait_recv()
    by_y = blend([stat(sma), stat(sb)], smb)
    m_stat = push(smb, sm, s_send.at[1], s_recv.at[1], mate)
    go(m_stat)
    m = [[push(unit(mb, i, h), unit(rm, i, h), m_send.at[i, h], m_recv.at[i, h], mate) for h in range(2)]
         for i in range(3)]
    f = [[push(unit(mc, i, h), rf.at[h * 16:h * 16 + 16, USED], f_send.at[i, h], f_recv.at[h], peer)
          for h in range(2)] for i, peer in enumerate((far_end, far_inner))]
    f_stat = [push(smc, sf, s_send.at[2 + i], s_recv.at[2], peer) for i, peer in enumerate((far_end, far_inner))]

    def y_step(i, h):
        b[i][h].wait_recv()
        merge(order[4 + i], by_y[h], [of(ma, 4 + i, h), of(rb, i, h)], into(mb, i, h))
        if i < 2:
            if_end(lambda: go(m[i][h], at_end))
        elif i == 2:
            go(m[i][h])

    by_half = []

    def m_start():
        m_stat.wait_recv()
        by_half.extend(blend([stat(smb), stat(sm)], smc))
        for copy in f_stat:
            go(copy, at_inner)

    def m_step(i, h):
        m[i][h].wait_recv()
        merge(order[4 + i], by_half[h], [of(mb, i, h), of(rm, i, h)], into(mc, i, h))
        go(f[i][h], at_inner)

    y_step(0, 0)
    y_step(0, 1)
    y_step(1, 0)
    y_step(1, 1)

    @if_inner
    def _():
        by_half.clear()
        m_start()
        m_step(0, 0)
        m_step(0, 1)
    y_step(2, 0)

    def again():
        by_half.clear()
        by_half.extend(blend([stat(smb), stat(sm)]))

    @if_inner
    def _():
        again()
        m_step(1, 0)
    y_step(2, 1)

    @if_inner
    def _():
        again()
        m_step(1, 1)
    y_step(3, 0)
    y_step(3, 1)

    if_end(m_stat.wait_recv)
    f_stat[0].wait_recv()
    by_z = blend([stat(smb), stat(sm), stat(sf)], divide=True)
    for h in range(2):
        m[2][h].wait_recv()
        f[0][h].wait_recv()

        def final(bb, value, h=h):
            fin[pl.ds(h * 128 + bb * 8, 8), :] = value

        merge(order[7], by_z[h], [of(mb, 3, h), of(rm, 2, h), lambda bb, h=h: rf[h * 16 + bb]], final)
    for t in range(7):
        lhs[mine, t * 128:(t + 1) * 128] = fin[pl.ds(t, 32, stride=8), :].astype(BF16)
    d_copy = push(lhs.at[mine], lhs.at[mine], d_send, d_recv, partner)
    go(d_copy)
    for copy in w_copies:
        copy.wait()
    push(lhs.at[theirs], lhs.at[theirs], d_send, d_recv, partner).wait_recv()

    def rows_of(j):
        return pl.ds(pl.multiple_of(j * 8, 8), 8)

    quarter = HALF // 2

    def cols_of(h):
        return pl.ds(h * quarter, quarter)

    b2 = [[push(p.at[rows_of(order[i]), cols_of(h)], rb2.at[i, h], b2_send.at[i, h], b2_recv.at[i, h], y_peer)
           for h in range(2)] for i in range(4)]
    m2 = [[push(mb2.at[i, h], rm2.at[i, h], m2_send.at[i, h], m2_recv.at[i, h], mate) for h in range(2)]
          for i in range(3)]
    f2 = [[push(mc2.at[i, h], rf2.at[h], f2_send.at[i, h], f2_recv.at[h], peer) for h in range(2)]
          for i, peer in enumerate((far_end, far_inner))]
    for h in range(2):
        for n in range(2):
            at = h * quarter + n * (quarter // 2)
            p[:, at:at + quarter // 2] = jnp.dot(lhs[...], wbuf[:, at:at + quarter // 2], preferred_element_type=F32)
        for i in range(4):
            go(b2[i][h])

    def y2_step(i, h):
        b2[i][h].wait_recv()
        mb2[i, h] = p[rows_of(order[4 + i]), h * quarter:(h + 1) * quarter] + rb2[i, h]
        if i < 2:
            if_end(lambda: go(m2[i][h], at_end))
        elif i == 2:
            go(m2[i][h])

    def m2_step(i, h):
        m2[i][h].wait_recv()
        mc2[i, h] = mb2[i, h] + rm2[i, h]
        go(f2[i][h], at_inner)

    def part(j, c, h):
        return out.at[rows_of(j), pl.ds(pl.multiple_of(c * HALF + h * quarter, 128), quarter)]

    whole = Gather(me, lambda j, h: part(j, me.c, h), lambda j, h: part(j, 1 - me.c, h), sems)
    for h in range(2):
        for i in range(4):
            y2_step(i, h)
            if i == 2:
                @if_inner
                def _():
                    m2_step(0, h)
        if_inner(lambda: m2_step(1, h))
    for h in range(2):
        m2[2][h].wait_recv()
        f2[0][h].wait_recv()
        total = (mb2[3, h] + rm2[2, h]) + rf2[h]
        out[rows_of(me.j), pl.ds(pl.multiple_of(me.c * HALF + h * quarter, 128), quarter)] = total.astype(BF16)
        whole.start(h)
    whole.finish()
    for copy in started:
        copy.wait_send()

    @if_end
    def _():
        for copy in at_end:
            copy.wait_send()

    @if_inner
    def _():
        for copy in at_inner:
            copy.wait_send()


def dma(*shape):
    return pltpu.SemaphoreType.DMA(shape) if shape else pltpu.SemaphoreType.DMA


def solution(mesh):
    cache_spec = P('rep', 'seq', None, None)
    in_specs = (P('rep', None), P(), P(), P(), P('seq', None), cache_spec, cache_spec, P('rep'))
    out_specs = (P('rep', None), cache_spec, cache_spec)
    shape = jax.ShapeDtypeStruct

    def step(x, wq, wk, wv, wo, k, v, pos):
        cache = (64, 512, 128)
        g, wox, k2, v2 = pl.pallas_call(
            project_kernel,
            out_shape=[pltpu.VMEM((8, 9, 64, 128), BF16), shape((ROWS, HALF), BF16), pltpu.VMEM(cache, BF16),
                       pltpu.VMEM(cache, BF16)],
            in_specs=[HBM] * 7,
            out_specs=[VMEM, HBM, VMEM, VMEM],
            scratch_shapes=[pltpu.VMEM((64, D), BF16), pltpu.VMEM((D, 640), BF16), dma(), dma(2, CHUNKS, 2), dma(2), dma(),
                            dma()] + GATHER_SEMS,
            cost_estimate=pl.CostEstimate(flops=10 ** 10, bytes_accessed=10 ** 7, transcendentals=0),
            compiler_params=pltpu.CompilerParams(
                collective_id=1, has_side_effects=True, vmem_limit_bytes=32 * 2 ** 20),
            name='project',
        )(*[pltpu.with_memory_space_constraint(a, pltpu.HBM)
            for a in (x, wq, wk, wv, wo, k.reshape(cache), v.reshape(cache))])
        _, _, ko, vo, o, stats = pl.pallas_call(
            attend_kernel,
            out_shape=[pltpu.VMEM(cache, BF16), pltpu.VMEM(cache, BF16), shape(cache, BF16), shape(cache, BF16),
                       shape((8, 64, 8, 128), F32), shape((2, 4, 8, 128), F32)],
            in_specs=[SMEM, VMEM, VMEM, VMEM],
            out_specs=[VMEM, VMEM, HBM, HBM, VMEM, VMEM],
            input_output_aliases={2: 0, 3: 1},
            scratch_shapes=[pltpu.VMEM((64 * PITCH, 128), F32), pltpu.VMEM((8 * PITCH, 128), F32), dma(4), dma(4)],
            cost_estimate=pl.CostEstimate(flops=2 * 10 ** 9, bytes_accessed=4 * 10 ** 7, transcendentals=0),
            compiler_params=pltpu.CompilerParams(vmem_limit_bytes=30 * 2 ** 20),
            name='attend',
        )(pos, g, k2, v2)
        piece = (32, 8, 128)
        stat = pltpu.VMEM((2, 2, 8, 128), F32)

        def pieces(n):
            return pltpu.VMEM((n,) + piece, F32)

        def sums(n):
            return pltpu.VMEM((n, 2, 8, HALF // 2), F32)

        y = pl.pallas_call(
            combine_kernel,
            out_shape=shape((64, D), BF16),
            in_specs=[VMEM, VMEM, HBM, HBM],
            out_specs=VMEM,
            scratch_shapes=[
                pieces(8), stat, pieces(8), stat, pieces(4), stat, pieces(4), stat, pieces(3), stat, pieces(2), stat,
                pltpu.VMEM(piece, F32), stat,
                pltpu.VMEM((256, 128), F32), pltpu.VMEM((64, 896), BF16), pltpu.VMEM((896, HALF), BF16),
                pltpu.VMEM((64, HALF), F32), sums(4), sums(4), sums(3), sums(2), pltpu.VMEM((2, 8, HALF // 2), F32),
                dma(2), dma(9), dma(9), dma(4, 2), dma(4, 2), dma(3, 2), dma(3, 2), dma(2, 2), dma(2),
                dma(4), dma(3), dma(), dma(), dma(4, 2), dma(4, 2), dma(3, 2), dma(3, 2), dma(2, 2), dma(2),
            ] + GATHER_SEMS,
            cost_estimate=pl.CostEstimate(flops=10 ** 10, bytes_accessed=10 ** 7, transcendentals=0),
            compiler_params=pltpu.CompilerParams(
                collective_id=2, has_side_effects=True, vmem_limit_bytes=28 * 2 ** 20),
            name='combine',
        )(o, stats, pltpu.with_memory_space_constraint(wo, pltpu.HBM), wox)
        return y, ko.reshape(k.shape), vo.reshape(v.shape)

    return jax.shard_map(step, mesh=mesh, in_specs=in_specs, out_specs=out_specs, check_vma=False)
```

```python
import functools

import jax
import jax.numpy as jnp
from jax import lax
from jax.experimental import pallas as pl
from jax.experimental.pallas import tpu as pltpu
from jax.sharding import PartitionSpec as P

MESH = pl.DeviceIdType.MESH
F32, BF16 = jnp.float32, jnp.bfloat16
VMEM = pl.BlockSpec(memory_space=pltpu.VMEM)
HBM = pl.BlockSpec(memory_space=pltpu.HBM)
SMEM = pl.BlockSpec(memory_space=pltpu.SMEM)
LOWEST = float(jnp.finfo(jnp.float32).min)
LANES = 128
D = 7168
HALF = D // 2
ROWS = 448
CHUNKS = 4
GROUP = 1
SLICES = 4
PARTS = 4
USED = slice(0, 7)
BATCH = 16
PITCH = 65
CHUNK = D // CHUNKS


Y_STEPS = ('y00y01y10y11y20y21y02y03m00m01y12m10', 'y13m11y22m02y23m03y30m12y31m13y32y33')
OUT_STEPS = ('y00y10y01y11y02m00y12m10y03m01y13m11y20m02', 'y21m12y22m03y23m13y30f00y31f01y32f02y33f03')


def read_steps(lines):
    return [('ymf'.index(line[n]), int(line[n + 1]), int(line[n + 2])) for line in lines
            for n in range(0, len(line), 3)]


class Place:
    def __init__(self):
        self.rep = lax.axis_index('rep')
        seq = lax.axis_index('seq')
        self.z = seq // 4
        self.y = lax.rem(seq // 2, 2)
        self.c = lax.rem(seq, 2)
        self.j = seq // 2

    def at(self, z, y, c):
        return (self.rep, (z * 2 + y) * 2 + c)

    def others(self):
        z = self.z
        low = 1 - z // 2
        return [low * 3, 1 + low, z + 1 - 2 * lax.rem(z, 2), z]

    def inner(self):
        return jnp.logical_and(self.z >= 1, self.z <= 2)

    def greet(self):
        barrier = pltpu.get_barrier_semaphore()
        peers = [self.at(self.z, self.y, 1 - self.c), self.at(self.z, 1 - self.y, self.c)]
        peers += [self.at(zz, self.y, self.c) for zz in self.others()[:3]]
        for peer in peers:
            pl.semaphore_signal(barrier, inc=1, device_id=peer, device_id_type=MESH)
        pl.semaphore_wait(barrier, len(peers))


def push(src, dst, send, recv, device):
    copy = pltpu.make_async_remote_copy(
        src_ref=src, dst_ref=dst, send_sem=send, recv_sem=recv, device_id=device, device_id_type=MESH)
    return copy


class Gather:
    def __init__(self, me, region, other, sems):
        self.me, self.region, self.other = me, region, other
        self.z_send, self.z_recv, self.y_send, self.y_recv, self.c_send, self.c_recv = sems
        self.zs = me.others()

    def go(self, copy):
        copy.start()

    def along_z(self, h, i, j, arrival=False):
        src = self.region(j, h)
        slot = i if arrival or i == 2 else lax.rem((self.me.z + 1) // 2, 2)
        return push(src, src, self.z_send.at[h, i], self.z_recv.at[h, slot],
                    self.me.at(self.zs[i], self.me.y, self.me.c))

    def across_y(self, h, i, j):
        src = self.region(j, h)
        return push(src, src, self.y_send.at[h, i], self.y_recv.at[h, i],
                    self.me.at(self.me.z, 1 - self.me.y, self.me.c))

    def to_core(self, h, i, src):
        return push(src, src, self.c_send.at[h, i], self.c_recv.at[h, i],
                    self.me.at(self.me.z, self.me.y, 1 - self.me.c))

    def start(self, h):
        for i in range(3):
            self.go(self.along_z(h, i, self.me.j))
        self.go(self.across_y(h, 3, self.me.j))
        self.go(self.to_core(h, 3, self.region(self.me.j, h)))

    def near(self, i):
        return self.zs[i] * 2 + self.me.y

    def far(self, i):
        return self.zs[i] * 2 + 1 - self.me.y

    def from_z(self, h):
        for i in (2, 1, 0):
            self.along_z(h, i, self.near(i), arrival=True).wait_recv()
            self.go(self.across_y(h, i, self.near(i)))
            self.go(self.to_core(h, i, self.region(self.near(i), h)))

    def from_y(self, h):
        for i in (3, 2, 1, 0):
            self.across_y(h, i, self.far(i)).wait_recv()
            self.go(self.to_core(h, 4 + i, self.region(self.far(i), h)))

    def from_core(self, h):
        for i in (3, 2, 1, 0):
            self.to_core(h, i, self.other(self.near(i), h)).wait_recv()
            self.to_core(h, 4 + i, self.other(self.far(i), h)).wait_recv()

    def sent(self, h):
        for i in range(3):
            self.along_z(h, i, self.me.j).wait_send()
        for i in range(4):
            self.across_y(h, i, self.near(i)).wait_send()
            self.to_core(h, i, self.region(self.near(i), h)).wait_send()
            self.to_core(h, 4 + i, self.region(self.far(i), h)).wait_send()


def gather_sems(parts):
    return [pltpu.SemaphoreType.DMA((parts, n)) for n in (3, 3, 4, 4, 8, 8)]


TILES = ((0, 5), (5, 4))


def step_kernel(pos_in, x_in, wq, wk, wv, wo, k_in, v_in, out, k, v, kn, vn,
                g, x, wbuf, qs, vs, o, stats, ra, sa, ma, sma, rb, sb, mb, smb, rm, sm, mc, smc, rf, sf, fin, lhs,
                wbuf2, p, rb2, mb2, rm2, mc2, rf2,
                pos, pos_sem, x_sem, w_sem, kv_sem, wo_sem, swap_send, swap_recv, a_send, a_recv, b_send, b_recv, m_send, m_recv,
                f_send, f_recv, as_send, as_recv, bs_send, bs_recv, ms_send, ms_recv, fs_send, fs_recv,
                d_send, d_recv, b2_send, b2_recv, m2_send, m2_recv, f2_send, f2_recv, *sems):
    me = Place()
    zs = me.others()
    partner = me.at(me.z, me.y, 1 - me.c)
    y_peer = me.at(me.z, 1 - me.y, me.c)
    far_end, far_inner, mate = [me.at(zs[i], me.y, me.c) for i in range(3)]
    mine = pl.ds(pl.multiple_of(me.c * 32, 32), 32)
    theirs = pl.ds(pl.multiple_of((1 - me.c) * 32, 32), 32)
    started, at_end, at_inner = [], [], []

    def go(copy, kept=started):
        copy.start()
        kept.append(copy)

    def if_inner(f):
        pl.when(me.inner())(f)

    def if_end(f):
        pl.when(jnp.logical_not(me.inner()))(f)

    x_copy = pltpu.make_async_copy(x_in, x, x_sem)
    pos_copy = pltpu.make_async_copy(pos_in, pos, pos_sem)
    pos_copy.start()
    cache = []
    for i in range(SLICES):
        bs = slice(i * 64 // SLICES, (i + 1) * 64 // SLICES)
        cache += [pltpu.make_async_copy(k_in.at[bs], k.at[bs], kv_sem.at[0, i]),
                  pltpu.make_async_copy(v_in.at[bs], v.at[bs], kv_sem.at[1, i])]

    def weights(c, i):
        rows = pl.ds(i * CHUNK, CHUNK)
        if c == 0:
            parts = [(wq, me.j * 896, 640)]
        else:
            parts = [(wq, me.j * 896 + 640, 256), (wk, me.j * LANES, LANES), (wv, me.j * LANES, LANES)]
        at, copies = 0, []
        for n, (w, col, width) in enumerate(parts):
            copies.append(pltpu.make_async_copy(w.at[rows, pl.ds(pl.multiple_of(col, LANES), width)],
                                                wbuf.at[rows, at:at + width], w_sem.at[i, n]))
            at += width
        return copies

    for c in range(2):
        @pl.when(me.c == c)
        def _(c=c):
            for i in range(CHUNKS):
                for copy in weights(c, i):
                    copy.start()
                if i == 0:
                    x_copy.start()

    me.greet()
    x_copy.wait()
    for c in range(2):
        @pl.when(me.c == c)
        def _(c=c):
            lo, n = TILES[c]
            acc = jnp.zeros((64, n * LANES), F32)
            rows = GROUP * CHUNK
            for i in range(CHUNKS // GROUP):
                for u in range(GROUP):
                    for copy in weights(c, i * GROUP + u):
                        copy.wait()
                acc += jnp.dot(x[:, i * rows:(i + 1) * rows], wbuf[i * rows:(i + 1) * rows, :n * LANES],
                               preferred_element_type=F32)
            for h in range(2):
                for q in range(2):
                    for t in range(n):
                        g[h, me.j, lo + t, q * 16:q * 16 + 16] = acc[
                            q * 32 + h * 16:q * 32 + h * 16 + 16, t * LANES:(t + 1) * LANES].astype(BF16)

    wo_copy = pltpu.make_async_copy(wo.at[:, pl.ds(pl.multiple_of(me.c * HALF, LANES), HALF)],
                                    wbuf2.at[pl.ds(pl.multiple_of(me.c * ROWS, 64), ROWS)], wo_sem)
    swap = push(wo.at[:, pl.ds(pl.multiple_of((1 - me.c) * HALF, LANES), HALF)],
                wbuf2.at[pl.ds(pl.multiple_of(me.c * ROWS, 64), ROWS)], swap_send, swap_recv, partner)

    def begin_caches():
        for copy in cache:
            copy.start()
        wo_copy.start()
        swap.start()

    def inputs(f):
        for c in range(2):
            @pl.when(me.c == c)
            def _(c=c):
                lo, n = TILES[c]
                lo2, n2 = TILES[1 - c]
                f(Gather(me, lambda j, h: g.at[h, j, lo:lo + n], lambda j, h: g.at[h, j, lo2:lo2 + n2], sems[:6]))

    def gather_first(w):
        w.start(0)
        w.start(1)

    def gather_relay(w):
        w.from_z(0)
        w.from_z(1)
        w.from_y(0)
        w.from_core(0)

    def gather_last(w):
        w.from_core(1)
        w.sent(0)
        w.sent(1)

    inputs(gather_first)
    begin_caches()
    inputs(gather_relay)
    for copy in cache:
        copy.wait()
    pos_copy.wait()

    first = lax.axis_index('seq') * 64
    s_of = lax.broadcasted_iota(jnp.int32, (8, LANES), 1) // 8
    lane = lax.broadcasted_iota(jnp.int32, (8, 512), 1)
    is_head = [lax.rem(lane, 8) == n for n in range(8)]
    at_of = lane // 8
    row_of = lax.broadcasted_iota(jnp.int32, (512, LANES), 0) // 8

    def spread(h):
        def head(j, _):
            for t in range(8):
                qs[pl.ds((j * 8 + t) * PITCH + h * 32, 32), :] = g[h, j, t].astype(F32)
            vs[pl.ds(j * PITCH + h * 32, 32), :] = g[h, j, 8].astype(F32)
            return 0

        lax.fori_loop(0, 8, head, 0)

        def news(e, _):
            at = h * 32 + e
            for to, new in ((kn, qs[pl.ds(7 * PITCH + at, 8, stride=8 * PITCH), :]),
                            (vn, vs[pl.ds(at, 8, stride=PITCH), :])):
                to[at] = jnp.concatenate([new, new], axis=0).astype(BF16)
            return 0

        lax.fori_loop(0, 32, news, 0, unroll=8)

    def with_new(ref, b, new, limit):
        return jnp.where(row_of == limit, jnp.concatenate([new] * 32, axis=0), ref[b])

    def scores(b, at):
        q = qs[pl.ds(at, 64, stride=PITCH), :].astype(BF16)
        limit = pos[b] - first
        s = lax.dot_general(q, with_new(k, b, kn[at], limit), (((1,), (1,)), ((), ())), preferred_element_type=F32)
        t = s[0:8]
        for hd in range(1, 8):
            t = jnp.where(is_head[hd], s[hd * 8:hd * 8 + 8], t)
        valid = at_of <= limit
        return jnp.where(valid, t * (LANES ** -0.5), LOWEST), valid

    def quarters(a):
        return [a[:, n * LANES:(n + 1) * LANES] for n in range(4)]

    def soften(batch):
        m = []
        for t, _ in batch:
            q = quarters(t)
            m.append(jnp.maximum(jnp.maximum(q[0], q[1]), jnp.maximum(q[2], q[3])))
        for shift in (8, 16, 32, 64):
            turned = [pltpu.roll(a, shift, 1) for a in m]
            m = [jnp.maximum(a, b) for a, b in zip(m, turned)]
        e = [jnp.where(valid, jnp.exp(t - jnp.concatenate([a] * 4, axis=1)), 0.0) for (t, valid), a in zip(batch, m)]
        l = []
        for w in e:
            q = quarters(w)
            l.append((q[0] + q[1]) + (q[2] + q[3]))
        for shift in (8, 16, 32, 64):
            turned = [pltpu.roll(a, shift, 1) for a in l]
            l = [a + b for a, b in zip(l, turned)]
        return m, l, e

    def values(b, at, e):
        w = jnp.concatenate([jnp.where(is_head[hd], e, 0.0) for hd in range(8)], axis=0).astype(BF16)
        ob = jnp.dot(w, with_new(v, b, vn[at], pos[b] - first), preferred_element_type=F32)
        for hd in range(8):
            o[hd, b] = ob[hd * 8:hd * 8 + 8]

    def attend(h, q):
        places = [(q * 32 + h * 16 + e, h * 32 + q * 16 + e) for e in range(16)]
        ahead = [scores(*place) for place in places[:BATCH]]
        ms = ls = jnp.zeros((8, LANES), F32)
        for i in range(16 // BATCH):
            batch, ahead = ahead, []
            if i + 1 < 16 // BATCH:
                ahead = [scores(*place) for place in places[(i + 1) * BATCH:(i + 2) * BATCH]]
            m, l, w = soften(batch)
            for e in range(BATCH):
                bb = i * BATCH + e
                values(*places[bb], w[e])
                here = s_of == bb
                ms, ls = jnp.where(here, m[e], ms), jnp.where(here, l[e], ls)
        stats[0, q * 2 + h] = ms
        stats[1, q * 2 + h] = ls

    order = [zs[i] * 2 + 1 - me.y for i in range(4)] + [zs[i] * 2 + me.y for i in range(4)]
    a_stat = [push(stats.at[:, (1 - me.c) * 2 + h], sa.at[:, h], as_send.at[h], as_recv.at[h], partner)
              for h in range(2)]
    a = [[push(o.at[order[i], pl.ds((1 - me.c) * 32 + h * 16, 16), USED], ra.at[i, h * 16:h * 16 + 16, USED],
               a_send.at[i, h], a_recv.at[i, h], partner) for h in range(2)] for i in range(8)]

    def exchange(h):
        go(a_stat[h])
        for i in range(8):
            go(a[i][h])

    def weights_of(m_list, l_list):
        top = m_list[0]
        for m in m_list[1:]:
            top = jnp.maximum(top, m)
        scale = [jnp.exp(m - top) for m in m_list]
        total = scale[0] * l_list[0]
        for f, l in zip(scale[1:], l_list[1:]):
            total = total + f * l
        return top, total, scale

    def blend(stat_refs, h, out_ref=None, divide=False):
        top, total, scale = weights_of([r(0, h) for r in stat_refs], [r(1, h) for r in stat_refs])
        if out_ref is not None:
            out_ref[0, h], out_ref[1, h] = top, total
        return [f / total for f in scale] if divide else scale

    def merge(head, q, factors, sources, store):
        turned = [pltpu.roll(f, lax.rem(LANES - head, LANES), 1) for f in factors]
        for bb in range(8):
            total = None
            lane0 = (q % 2 * 8 + bb) * 8
            for f, source in zip(turned, sources):
                term = source(q * 8 + bb) * jnp.broadcast_to(f[:, lane0:lane0 + 1], (8, LANES))
                total = term if total is None else total + term
            store(q * 8 + bb, total)

    def of(ref, i):
        return lambda b: ref[i, b]

    def into(ref, i):
        def store(b, value):
            ref[i, b] = value
        return store

    def unit(ref, i, q):
        return ref.at[i, q * 8:q * 8 + 8, USED]

    def stat(ref):
        return lambda s, h: ref[s, h]

    b_stat = [push(sma.at[:, h], sb.at[:, h], bs_send.at[h], bs_recv.at[h], y_peer) for h in range(2)]
    b = [[push(unit(ma, i, q), unit(rb, i, q), b_send.at[i, q], b_recv.at[i, q], y_peer) for q in range(PARTS)]
         for i in range(4)]
    by_core = [None, None]

    def core_step(h, some):
        if by_core[h] is None:
            a_stat[h].wait_recv()
            by_core[h] = blend([lambda s, h: stats[s, me.c * 2 + h], stat(sa)], h, sma)
            go(b_stat[h])
        for i in some:
            a[i][h].wait_recv()
        for i in some:
            for q in (2 * h, 2 * h + 1):
                merge(order[i], q, by_core[h], [lambda bb, i=i: o[order[i], me.c * 32 + bb], of(ra, i)], into(ma, i))
        for i in some:
            if i < 4:
                go(b[i][2 * h])
                go(b[i][2 * h + 1])

    spread(0)
    attend(0, 1 - me.c)
    inputs(lambda w: w.from_y(1))
    exchange(0)
    attend(0, me.c)
    core_step(0, range(3))
    inputs(gather_last)
    spread(1)
    attend(1, 1 - me.c)
    exchange(1)
    attend(1, me.c)
    core_step(1, range(3))
    core_step(0, range(3, 8))
    core_step(1, range(3, 8))

    m_stat = [push(smb.at[:, h], sm.at[:, h], ms_send.at[h], ms_recv.at[h], mate) for h in range(2)]
    m = [[push(unit(mb, i, q), unit(rm, i, q), m_send.at[i, q], m_recv.at[i, q], mate) for q in range(PARTS)]
         for i in range(3)]
    f = [[push(unit(mc, i, q), rf.at[q * 8:q * 8 + 8, USED], f_send.at[i, q], f_recv.at[q], peer)
          for q in range(PARTS)] for i, peer in enumerate((far_end, far_inner))]
    f_stat = [[push(smc.at[:, h], sf.at[:, h], fs_send.at[i, h], fs_recv.at[h], peer) for h in range(2)]
              for i, peer in enumerate((far_end, far_inner))]
    by_y = [None, None]

    def y_step(i, q):
        h = q // 2
        if by_y[h] is None:
            b_stat[h].wait_recv()
            by_y[h] = blend([stat(sma), stat(sb)], h, smb)
            go(m_stat[h])
        b[i][q].wait_recv()
        merge(order[4 + i], q, by_y[h], [of(ma, 4 + i), of(rb, i)], into(mb, i))
        if i < 2:
            if_end(lambda: go(m[i][q], at_end))
        elif i == 2:
            go(m[i][q])

    def m_step(i, q):
        h = q // 2
        opens = i == 0 and q % 2 == 0
        if opens:
            m_stat[h].wait_recv()
        factors = blend([stat(smb), stat(sm)], h, smc if opens else None)
        if opens:
            for copy in f_stat:
                go(copy[h], at_inner)
        m[i][q].wait_recv()
        merge(order[4 + i], q, factors, [of(mb, i), of(rm, i)], into(mc, i))
        go(f[i][q], at_inner)

    for inner, i, q in read_steps(Y_STEPS):
        if not inner:
            y_step(i, q)
        else:
            if_inner(lambda: m_step(i, q))

    for q in range(PARTS):
        h = q // 2
        if q % 2 == 0:
            if_end(m_stat[h].wait_recv)
            f_stat[0][h].wait_recv()
            by_z = blend([stat(smb), stat(sm), stat(sf)], h, divide=True)
        m[2][q].wait_recv()
        f[0][q].wait_recv()

        def final(b, value):
            fin[pl.ds(b * 8, 8), :] = value

        merge(order[7], q, by_z, [of(mb, 3), of(rm, 2), lambda b: rf[b]], final)
    for t in range(7):
        lhs[mine, t * LANES:(t + 1) * LANES] = fin[pl.ds(t, 32, stride=8), :].astype(BF16)
    d_copy = push(lhs.at[mine], lhs.at[mine], d_send, d_recv, partner)
    go(d_copy)
    wo_copy.wait()
    swap.wait_send()
    push(wo.at[:, pl.ds(0, HALF)], wbuf2.at[pl.ds(pl.multiple_of((1 - me.c) * ROWS, 64), ROWS)], swap_send, swap_recv,
         partner).wait_recv()
    push(lhs.at[theirs], lhs.at[theirs], d_send, d_recv, partner).wait_recv()

    def rows_of(j):
        return pl.ds(pl.multiple_of(j * 8, 8), 8)

    width = HALF // PARTS

    def cols_of(q):
        return pl.ds(q * width, width)

    b2 = [[push(p.at[rows_of(order[i]), cols_of(q)], rb2.at[i, q], b2_send.at[i, q], b2_recv.at[i, q], y_peer)
           for q in range(PARTS)] for i in range(4)]
    m2 = [[push(mb2.at[i, q], rm2.at[i, q], m2_send.at[i, q], m2_recv.at[i, q], mate) for q in range(PARTS)]
          for i in range(3)]
    f2 = [[push(mc2.at[i, q], rf2.at[q], f2_send.at[i, q], f2_recv.at[q], peer) for q in range(PARTS)]
          for i, peer in enumerate((far_end, far_inner))]
    for q in range(PARTS):
        at = q * width
        p[:, at:at + width] = jnp.dot(lhs[...], wbuf2[:, at:at + width], preferred_element_type=F32)
        for i in range(2):
            go(b2[i][q])
    for i in range(2, 4):
        for q in range(PARTS):
            go(b2[i][q])

    def y2_step(i, q):
        b2[i][q].wait_recv()
        mb2[i, q] = p[rows_of(order[4 + i]), q * width:(q + 1) * width] + rb2[i, q]
        if i < 2:
            if_end(lambda: go(m2[i][q], at_end))
        elif i == 2:
            go(m2[i][q])

    def m2_step(i, q):
        m2[i][q].wait_recv()
        mc2[i, q] = mb2[i, q] + rm2[i, q]
        go(f2[i][q], at_inner)

    def part(j, c, q):
        return out.at[rows_of(j), pl.ds(pl.multiple_of(c * HALF + q * width, LANES), width)]

    whole = Gather(me, lambda j, q: part(j, me.c, q), lambda j, q: part(j, 1 - me.c, q), sems[6:])

    def finish(q):
        m2[2][q].wait_recv()
        f2[0][q].wait_recv()
        total = (mb2[3, q] + rm2[2, q]) + rf2[q]
        out[rows_of(me.j), pl.ds(pl.multiple_of(me.c * HALF + q * width, LANES), width)] = total.astype(BF16)
        whole.start(q)

    for kind, i, q in read_steps(OUT_STEPS):
        if kind == 0:
            y2_step(i, q)
        elif kind == 1:
            if_inner(lambda: m2_step(i, q))
        else:
            finish(q)
    for q in range(PARTS):
        whole.from_z(q)
    for q in range(PARTS):
        whole.from_y(q)
    for q in range(PARTS):
        whole.from_core(q)
    for q in range(PARTS):
        whole.sent(q)
    for copy in started:
        copy.wait_send()

    @if_end
    def _():
        for copy in at_end:
            copy.wait_send()

    @if_inner
    def _():
        for copy in at_inner:
            copy.wait_send()


def write_kernel(pos, kn, vn, k_in, v_in, k, v, ko, vo, k_sem, v_sem):
    first = lax.axis_index('seq') * 64

    def out(i):
        bs = pl.ds(i * 16, 16)
        return [pltpu.make_async_copy(k.at[bs], ko.at[bs], k_sem.at[i]),
                pltpu.make_async_copy(v.at[bs], vo.at[bs], v_sem.at[i])]

    for i in range(4):
        for e in range(16):
            b = i * 16 + e
            at = lax.rem(i, 2) * 32 + i // 2 * 16 + e
            row = pos[b] - first
            here = jnp.logical_and(row >= 0, row < 64)
            rows = pl.ds(pl.multiple_of(jnp.clip(row, 0, 63) * 8, 8), 8)
            k[b, rows, :] = jnp.where(here, kn[at, 0:8], k[b, rows, :])
            v[b, rows, :] = jnp.where(here, vn[at, 0:8], v[b, rows, :])
        for copy in out(i):
            copy.start()
    for i in range(4):
        for copy in out(i):
            copy.wait()


def dma(*shape):
    return pltpu.SemaphoreType.DMA(shape) if shape else pltpu.SemaphoreType.DMA


def solution(mesh):
    cache_spec = P('rep', 'seq', None, None)
    in_specs = (P('rep', None), P(), P(), P(), P('seq', None), cache_spec, cache_spec, P('rep'))
    out_specs = (P('rep', None), cache_spec, cache_spec)
    shape = jax.ShapeDtypeStruct

    def step(x, wq, wk, wv, wo, k, v, pos):
        cache = (64, 512, LANES)
        rows = pltpu.VMEM((64, 16, LANES), BF16)
        piece = (32, 8, LANES)
        stat = pltpu.VMEM((2, 2, 8, LANES), F32)

        def pieces(n):
            return pltpu.VMEM((n,) + piece, F32)

        def sums(n):
            return pltpu.VMEM((n, PARTS, 8, HALF // PARTS), F32)

        held = [pltpu.with_memory_space_constraint(a, pltpu.HBM)
                for a in (pos, x, wq, wk, wv, wo, k.reshape(cache), v.reshape(cache))]
        y, k2, v2, kn, vn = pl.pallas_call(
            step_kernel,
            out_shape=[pltpu.VMEM((64, D), BF16), pltpu.VMEM(cache, BF16), pltpu.VMEM(cache, BF16), rows, rows],
            in_specs=[HBM] * 8,
            out_specs=[VMEM] * 5,
            scratch_shapes=[
                pltpu.VMEM((2, 8, 9, 32, LANES), BF16), pltpu.VMEM((64, D), BF16), pltpu.VMEM((D, 640), BF16),
                pltpu.VMEM((64 * PITCH, LANES), F32), pltpu.VMEM((8 * PITCH, LANES), F32),
                pltpu.VMEM((8, 64, 8, LANES), F32), pltpu.VMEM((2, 4, 8, LANES), F32),
                pieces(8), stat, pieces(8), stat, pieces(4), stat, pieces(4), stat, pieces(3), stat, pieces(2), stat,
                pltpu.VMEM(piece, F32), stat,
                pltpu.VMEM((256, LANES), F32), pltpu.VMEM((64, 896), BF16), pltpu.VMEM((896, HALF), BF16),
                pltpu.VMEM((64, HALF), F32), sums(4), sums(4), sums(3), sums(2), pltpu.VMEM((PARTS, 8, HALF // PARTS), F32),
                pltpu.SMEM((64,), jnp.int32), dma(), dma(), dma(CHUNKS, 3), dma(2, SLICES), dma(), dma(), dma(),
                dma(8, 2), dma(8, 2), dma(4, PARTS), dma(4, PARTS), dma(3, PARTS), dma(3, PARTS), dma(2, PARTS), dma(PARTS),
                dma(2), dma(2), dma(2), dma(2), dma(2), dma(2), dma(2, 2), dma(2),
                dma(), dma(), dma(4, PARTS), dma(4, PARTS), dma(3, PARTS), dma(3, PARTS), dma(2, PARTS), dma(PARTS),
            ] + gather_sems(2) + gather_sems(PARTS),
            cost_estimate=pl.CostEstimate(flops=10 ** 10, bytes_accessed=10 ** 7, transcendentals=0),
            compiler_params=pltpu.CompilerParams(
                collective_id=1, has_side_effects=True, vmem_limit_bytes=36 * 2 ** 20),
            name='attend_step',
        )(*held)
        _, _, ko, vo = pl.pallas_call(
            write_kernel,
            out_shape=[pltpu.VMEM(cache, BF16), pltpu.VMEM(cache, BF16), shape(cache, BF16), shape(cache, BF16)],
            in_specs=[SMEM, VMEM, VMEM, VMEM, VMEM],
            out_specs=[VMEM, VMEM, HBM, HBM],
            input_output_aliases={3: 0, 4: 1},
            scratch_shapes=[dma(4), dma(4)],
            cost_estimate=pl.CostEstimate(flops=10 ** 9, bytes_accessed=4 * 10 ** 7, transcendentals=0),
            compiler_params=pltpu.CompilerParams(vmem_limit_bytes=30 * 2 ** 20),
            name='write_caches',
        )(pos, kn, vn, k2, v2)
        return y, ko.reshape(k.shape), vo.reshape(v.shape)

    return jax.shard_map(step, mesh=mesh, in_specs=in_specs, out_specs=out_specs, check_vma=False)
```

```python
import functools

import jax
import jax.numpy as jnp
from jax import lax
from jax.experimental import pallas as pl
from jax.experimental.pallas import tpu as pltpu
from jax.sharding import PartitionSpec as P

MESH = pl.DeviceIdType.MESH
F32, BF16 = jnp.float32, jnp.bfloat16
VMEM = pl.BlockSpec(memory_space=pltpu.VMEM)
HBM = pl.BlockSpec(memory_space=pltpu.HBM)
SMEM = pl.BlockSpec(memory_space=pltpu.SMEM)
LOWEST = float(jnp.finfo(jnp.float32).min)
LANES = 128
D = 7168
HALF = D // 2
ROWS = 448
CHUNKS = 4
GROUP = 1
SLICES = 4
PARTS = 4
USED = slice(0, 7)
BATCH = 16
PITCH = 65
CHUNK = D // CHUNKS


Y_STEPS = ('y00y01y10y11y20y21y02y03m00m01y12m10', 'y13m11y22m02y23m03y30m12y31m13y32y33')
OUT_STEPS = ('y00y10y01y11y02m00y12m10y03m01y13m11y20m02', 'y21m12y22m03y23m13y30f00y31f01y32f02y33f03')


def read_steps(lines):
    return [('ymf'.index(line[n]), int(line[n + 1]), int(line[n + 2])) for line in lines
            for n in range(0, len(line), 3)]


class Place:
    def __init__(self):
        self.rep = lax.axis_index('rep')
        seq = lax.axis_index('seq')
        self.z = seq // 4
        self.y = lax.rem(seq // 2, 2)
        self.c = lax.rem(seq, 2)
        self.j = seq // 2

    def at(self, z, y, c):
        return (self.rep, (z * 2 + y) * 2 + c)

    def others(self):
        z = self.z
        low = 1 - z // 2
        return [low * 3, 1 + low, z + 1 - 2 * lax.rem(z, 2), z]

    def inner(self):
        return jnp.logical_and(self.z >= 1, self.z <= 2)

    def greet(self):
        barrier = pltpu.get_barrier_semaphore()
        peers = [self.at(self.z, self.y, 1 - self.c), self.at(self.z, 1 - self.y, self.c)]
        peers += [self.at(zz, self.y, self.c) for zz in self.others()[:3]]
        for peer in peers:
            pl.semaphore_signal(barrier, inc=1, device_id=peer, device_id_type=MESH)
        pl.semaphore_wait(barrier, len(peers))


def push(src, dst, send, recv, device):
    copy = pltpu.make_async_remote_copy(
        src_ref=src, dst_ref=dst, send_sem=send, recv_sem=recv, device_id=device, device_id_type=MESH)
    return copy


class Gather:
    def __init__(self, me, region, other, sems):
        self.me, self.region, self.other = me, region, other
        self.z_send, self.z_recv, self.y_send, self.y_recv, self.c_send, self.c_recv = sems
        self.zs = me.others()

    def go(self, copy):
        copy.start()

    def along_z(self, h, i, j, arrival=False):
        src = self.region(j, h)
        slot = i if arrival or i == 2 else lax.rem((self.me.z + 1) // 2, 2)
        return push(src, src, self.z_send.at[h, i], self.z_recv.at[h, slot],
                    self.me.at(self.zs[i], self.me.y, self.me.c))

    def across_y(self, h, i, j):
        src = self.region(j, h)
        return push(src, src, self.y_send.at[h, i], self.y_recv.at[h, i],
                    self.me.at(self.me.z, 1 - self.me.y, self.me.c))

    def to_core(self, h, i, src):
        return push(src, src, self.c_send.at[h, i], self.c_recv.at[h, i],
                    self.me.at(self.me.z, self.me.y, 1 - self.me.c))

    def start(self, h):
        for i in range(3):
            self.go(self.along_z(h, i, self.me.j))
        self.go(self.across_y(h, 3, self.me.j))
        self.go(self.to_core(h, 3, self.region(self.me.j, h)))

    def near(self, i):
        return self.zs[i] * 2 + self.me.y

    def far(self, i):
        return self.zs[i] * 2 + 1 - self.me.y

    def from_z(self, h):
        for i in (2, 1, 0):
            self.along_z(h, i, self.near(i), arrival=True).wait_recv()
            self.go(self.across_y(h, i, self.near(i)))
            self.go(self.to_core(h, i, self.region(self.near(i), h)))

    def from_y(self, h):
        for i in (3, 2, 1, 0):
            self.across_y(h, i, self.far(i)).wait_recv()
            self.go(self.to_core(h, 4 + i, self.region(self.far(i), h)))

    def from_core(self, h):
        for i in (3, 2, 1, 0):
            self.to_core(h, i, self.other(self.near(i), h)).wait_recv()
            self.to_core(h, 4 + i, self.other(self.far(i), h)).wait_recv()

    def sent(self, h):
        for i in range(3):
            self.along_z(h, i, self.me.j).wait_send()
        for i in range(4):
            self.across_y(h, i, self.near(i)).wait_send()
            self.to_core(h, i, self.region(self.near(i), h)).wait_send()
            self.to_core(h, 4 + i, self.region(self.far(i), h)).wait_send()


def gather_sems(parts):
    return [pltpu.SemaphoreType.DMA((parts, n)) for n in (3, 3, 4, 4, 8, 8)]


TILES = ((0, 5), (5, 4))


def step_kernel(pos_in, x_in, wq, wk, wv, wo, k_in, v_in, out, k, v, kn, vn,
                g, x, wbuf, qs, vs, o, stats, ra, sa, ma, sma, rb, sb, mb, smb, rm, sm, mc, smc, rf, sf, fin, lhs,
                wbuf2, p, rb2, mb2, rm2, mc2, rf2,
                pos, pos_sem, x_sem, w_sem, kv_sem, wo_sem, swap_send, swap_recv, a_send, a_recv, b_send, b_recv, m_send, m_recv,
                f_send, f_recv, as_send, as_recv, bs_send, bs_recv, ms_send, ms_recv, fs_send, fs_recv,
                d_send, d_recv, b2_send, b2_recv, m2_send, m2_recv, f2_send, f2_recv, *sems):
    me = Place()
    zs = me.others()
    partner = me.at(me.z, me.y, 1 - me.c)
    y_peer = me.at(me.z, 1 - me.y, me.c)
    far_end, far_inner, mate = [me.at(zs[i], me.y, me.c) for i in range(3)]
    mine = pl.ds(pl.multiple_of(me.c * 32, 32), 32)
    theirs = pl.ds(pl.multiple_of((1 - me.c) * 32, 32), 32)
    started, at_end, at_inner = [], [], []

    def go(copy, kept=started):
        copy.start()
        kept.append(copy)

    def if_inner(f):
        pl.when(me.inner())(f)

    def if_end(f):
        pl.when(jnp.logical_not(me.inner()))(f)

    x_copy = pltpu.make_async_copy(x_in, x, x_sem)
    pos_copy = pltpu.make_async_copy(pos_in, pos, pos_sem)
    pos_copy.start()
    cache = []
    for i in range(SLICES):
        bs = slice(i * 64 // SLICES, (i + 1) * 64 // SLICES)
        cache += [pltpu.make_async_copy(k_in.at[bs], k.at[bs], kv_sem.at[0, i]),
                  pltpu.make_async_copy(v_in.at[bs], v.at[bs], kv_sem.at[1, i])]

    def weights(c, i):
        rows = pl.ds(i * CHUNK, CHUNK)
        if c == 0:
            parts = [(wq, me.j * 896, 640)]
        else:
            parts = [(wq, me.j * 896 + 640, 256), (wk, me.j * LANES, LANES), (wv, me.j * LANES, LANES)]
        at, copies = 0, []
        for n, (w, col, width) in enumerate(parts):
            copies.append(pltpu.make_async_copy(w.at[rows, pl.ds(pl.multiple_of(col, LANES), width)],
                                                wbuf.at[rows, at:at + width], w_sem.at[i, n]))
            at += width
        return copies

    for c in range(2):
        @pl.when(me.c == c)
        def _(c=c):
            for i in range(CHUNKS):
                for copy in weights(c, i):
                    copy.start()
                if i == 0:
                    x_copy.start()

    me.greet()
    x_copy.wait()
    for c in range(2):
        @pl.when(me.c == c)
        def _(c=c):
            lo, n = TILES[c]
            acc = jnp.zeros((64, n * LANES), F32)
            rows = GROUP * CHUNK
            for i in range(CHUNKS // GROUP):
                for u in range(GROUP):
                    for copy in weights(c, i * GROUP + u):
                        copy.wait()
                acc += jnp.dot(x[:, i * rows:(i + 1) * rows], wbuf[i * rows:(i + 1) * rows, :n * LANES],
                               preferred_element_type=F32)
            for h in range(2):
                for q in range(2):
                    for t in range(n):
                        g[h, me.j, lo + t, q * 16:q * 16 + 16] = acc[
                            q * 32 + h * 16:q * 32 + h * 16 + 16, t * LANES:(t + 1) * LANES].astype(BF16)

    wo_copy = pltpu.make_async_copy(wo.at[:, pl.ds(pl.multiple_of(me.c * HALF, LANES), HALF)],
                                    wbuf2.at[pl.ds(pl.multiple_of(me.c * ROWS, 64), ROWS)], wo_sem)
    swap = push(wo.at[:, pl.ds(pl.multiple_of((1 - me.c) * HALF, LANES), HALF)],
                wbuf2.at[pl.ds(pl.multiple_of(me.c * ROWS, 64), ROWS)], swap_send, swap_recv, partner)

    def begin_caches():
        for copy in cache:
            copy.start()
        wo_copy.start()
        swap.start()

    def inputs(f):
        for c in range(2):
            @pl.when(me.c == c)
            def _(c=c):
                lo, n = TILES[c]
                lo2, n2 = TILES[1 - c]
                f(Gather(me, lambda j, h: g.at[h, j, lo:lo + n], lambda j, h: g.at[h, j, lo2:lo2 + n2], sems[:6]))

    def gather_first(w):
        w.start(0)
        w.start(1)

    def gather_relay(w):
        w.from_z(0)
        w.from_z(1)
        w.from_y(0)
        w.from_core(0)

    def gather_last(w):
        w.from_core(1)
        w.sent(0)
        w.sent(1)

    inputs(gather_first)
    begin_caches()
    inputs(gather_relay)
    for copy in cache:
        copy.wait()
    pos_copy.wait()

    first = lax.axis_index('seq') * 64
    s_of = lax.broadcasted_iota(jnp.int32, (8, LANES), 1) // 8
    lane = lax.broadcasted_iota(jnp.int32, (8, 512), 1)
    is_head = [lax.rem(lane, 8) == n for n in range(8)]
    at_of = lane // 8
    row_of = lax.broadcasted_iota(jnp.int32, (512, LANES), 0) // 8

    def spread(h):
        def head(j, _):
            for t in range(8):
                qs[pl.ds((j * 8 + t) * PITCH + h * 32, 32), :] = g[h, j, t].astype(F32)
            vs[pl.ds(j * PITCH + h * 32, 32), :] = g[h, j, 8].astype(F32)
            return 0

        lax.fori_loop(0, 8, head, 0)

        def news(e, _):
            at = h * 32 + e
            for to, new in ((kn, qs[pl.ds(7 * PITCH + at, 8, stride=8 * PITCH), :]),
                            (vn, vs[pl.ds(at, 8, stride=PITCH), :])):
                to[at] = jnp.concatenate([new, new], axis=0).astype(BF16)
            return 0

        lax.fori_loop(0, 32, news, 0, unroll=8)

    def with_new(ref, b, new, limit):
        return jnp.where(row_of == limit, jnp.concatenate([new] * 32, axis=0), ref[b])

    def scores(b, at):
        q = qs[pl.ds(at, 64, stride=PITCH), :].astype(BF16)
        limit = pos[b] - first
        s = lax.dot_general(q, with_new(k, b, kn[at], limit), (((1,), (1,)), ((), ())), preferred_element_type=F32)
        t = s[0:8]
        for hd in range(1, 8):
            t = jnp.where(is_head[hd], s[hd * 8:hd * 8 + 8], t)
        valid = at_of <= limit
        return jnp.where(valid, t * (LANES ** -0.5), LOWEST), valid

    def quarters(a):
        return [a[:, n * LANES:(n + 1) * LANES] for n in range(4)]

    def soften(batch):
        m = []
        for t, _ in batch:
            q = quarters(t)
            m.append(jnp.maximum(jnp.maximum(q[0], q[1]), jnp.maximum(q[2], q[3])))
        for shift in (8, 16, 32, 64):
            turned = [pltpu.roll(a, shift, 1) for a in m]
            m = [jnp.maximum(a, b) for a, b in zip(m, turned)]
        e = [jnp.where(valid, jnp.exp(t - jnp.concatenate([a] * 4, axis=1)), 0.0) for (t, valid), a in zip(batch, m)]
        l = []
        for w in e:
            q = quarters(w)
            l.append((q[0] + q[1]) + (q[2] + q[3]))
        for shift in (8, 16, 32, 64):
            turned = [pltpu.roll(a, shift, 1) for a in l]
            l = [a + b for a, b in zip(l, turned)]
        return m, l, e

    def values(b, at, e):
        w = jnp.concatenate([jnp.where(is_head[hd], e, 0.0) for hd in range(8)], axis=0).astype(BF16)
        ob = jnp.dot(w, with_new(v, b, vn[at], pos[b] - first), preferred_element_type=F32)
        for hd in range(8):
            o[hd, b] = ob[hd * 8:hd * 8 + 8]

    def attend(h, q):
        places = [(q * 32 + h * 16 + e, h * 32 + q * 16 + e) for e in range(16)]
        ahead = [scores(*place) for place in places[:BATCH]]
        ms = ls = jnp.zeros((8, LANES), F32)
        for i in range(16 // BATCH):
            batch, ahead = ahead, []
            if i + 1 < 16 // BATCH:
                ahead = [scores(*place) for place in places[(i + 1) * BATCH:(i + 2) * BATCH]]
            m, l, w = soften(batch)
            for e in range(BATCH):
                bb = i * BATCH + e
                values(*places[bb], w[e])
                here = s_of == bb
                ms, ls = jnp.where(here, m[e], ms), jnp.where(here, l[e], ls)
        stats[0, q * 2 + h] = ms
        stats[1, q * 2 + h] = ls

    order = [zs[i] * 2 + 1 - me.y for i in range(4)] + [zs[i] * 2 + me.y for i in range(4)]
    a_stat = [push(stats.at[:, (1 - me.c) * 2 + h], sa.at[:, h], as_send.at[h], as_recv.at[h], partner)
              for h in range(2)]
    a = [[push(o.at[order[i], pl.ds((1 - me.c) * 32 + h * 16, 16), USED], ra.at[i, h * 16:h * 16 + 16, USED],
               a_send.at[i, h], a_recv.at[i, h], partner) for h in range(2)] for i in range(8)]

    def exchange(h):
        go(a_stat[h])
        for i in range(8):
            go(a[i][h])

    def weights_of(m_list, l_list):
        top = m_list[0]
        for m in m_list[1:]:
            top = jnp.maximum(top, m)
        scale = [jnp.exp(m - top) for m in m_list]
        total = scale[0] * l_list[0]
        for f, l in zip(scale[1:], l_list[1:]):
            total = total + f * l
        return top, total, scale

    def blend(stat_refs, h, out_ref=None, divide=False):
        top, total, scale = weights_of([r(0, h) for r in stat_refs], [r(1, h) for r in stat_refs])
        if out_ref is not None:
            out_ref[0, h], out_ref[1, h] = top, total
        return [f / total for f in scale] if divide else scale

    def merge(head, q, factors, sources, store):
        turned = [pltpu.roll(f, lax.rem(LANES - head, LANES), 1) for f in factors]
        for bb in range(8):
            total = None
            lane0 = (q % 2 * 8 + bb) * 8
            for f, source in zip(turned, sources):
                term = source(q * 8 + bb) * jnp.broadcast_to(f[:, lane0:lane0 + 1], (8, LANES))
                total = term if total is None else total + term
            store(q * 8 + bb, total)

    def of(ref, i):
        return lambda b: ref[i, b]

    def into(ref, i):
        def store(b, value):
            ref[i, b] = value
        return store

    def unit(ref, i, q):
        return ref.at[i, q * 8:q * 8 + 8, USED]

    def stat(ref):
        return lambda s, h: ref[s, h]

    b_stat = [push(sma.at[:, h], sb.at[:, h], bs_send.at[h], bs_recv.at[h], y_peer) for h in range(2)]
    b = [[push(unit(ma, i, q), unit(rb, i, q), b_send.at[i, q], b_recv.at[i, q], y_peer) for q in range(PARTS)]
         for i in range(4)]
    by_core = [None, None]

    def core_step(h, some):
        if by_core[h] is None:
            a_stat[h].wait_recv()
            by_core[h] = blend([lambda s, h: stats[s, me.c * 2 + h], stat(sa)], h, sma)
            go(b_stat[h])
        for i in some:
            a[i][h].wait_recv()
        for i in some:
            for q in (2 * h, 2 * h + 1):
                merge(order[i], q, by_core[h], [lambda bb, i=i: o[order[i], me.c * 32 + bb], of(ra, i)], into(ma, i))
        for i in some:
            if i < 4:
                go(b[i][2 * h])
                go(b[i][2 * h + 1])

    spread(0)
    attend(0, 1 - me.c)
    inputs(lambda w: w.from_y(1))
    exchange(0)
    attend(0, me.c)
    core_step(0, range(3))
    inputs(gather_last)
    spread(1)
    attend(1, 1 - me.c)
    exchange(1)
    attend(1, me.c)
    core_step(1, range(3))
    core_step(0, range(3, 8))
    core_step(1, range(3, 8))

    m_stat = [push(smb.at[:, h], sm.at[:, h], ms_send.at[h], ms_recv.at[h], mate) for h in range(2)]
    m = [[push(unit(mb, i, q), unit(rm, i, q), m_send.at[i, q], m_recv.at[i, q], mate) for q in range(PARTS)]
         for i in range(3)]
    f = [[push(unit(mc, i, q), rf.at[q * 8:q * 8 + 8, USED], f_send.at[i, q], f_recv.at[q], peer)
          for q in range(PARTS)] for i, peer in enumerate((far_end, far_inner))]
    f_stat = [[push(smc.at[:, h], sf.at[:, h], fs_send.at[i, h], fs_recv.at[h], peer) for h in range(2)]
              for i, peer in enumerate((far_end, far_inner))]
    by_y = [None, None]

    def y_step(i, q):
        h = q // 2
        if by_y[h] is None:
            b_stat[h].wait_recv()
            by_y[h] = blend([stat(sma), stat(sb)], h, smb)
            go(m_stat[h])
        b[i][q].wait_recv()
        merge(order[4 + i], q, by_y[h], [of(ma, 4 + i), of(rb, i)], into(mb, i))
        if i < 2:
            if_end(lambda: go(m[i][q], at_end))
        elif i == 2:
            go(m[i][q])

    def m_step(i, q):
        h = q // 2
        opens = i == 0 and q % 2 == 0
        if opens:
            m_stat[h].wait_recv()
        factors = blend([stat(smb), stat(sm)], h, smc if opens else None)
        if opens:
            for copy in f_stat:
                go(copy[h], at_inner)
        m[i][q].wait_recv()
        merge(order[4 + i], q, factors, [of(mb, i), of(rm, i)], into(mc, i))
        go(f[i][q], at_inner)

    for inner, i, q in read_steps(Y_STEPS):
        if not inner:
            y_step(i, q)
        else:
            if_inner(lambda: m_step(i, q))

    for q in range(PARTS):
        h = q // 2
        if q % 2 == 0:
            if_end(m_stat[h].wait_recv)
            f_stat[0][h].wait_recv()
            by_z = blend([stat(smb), stat(sm), stat(sf)], h, divide=True)
        m[2][q].wait_recv()
        f[0][q].wait_recv()

        def final(b, value):
            fin[pl.ds(b * 8, 8), :] = value

        merge(order[7], q, by_z, [of(mb, 3), of(rm, 2), lambda b: rf[b]], final)
    for t in range(7):
        lhs[mine, t * LANES:(t + 1) * LANES] = fin[pl.ds(t, 32, stride=8), :].astype(BF16)
    d_copy = push(lhs.at[mine], lhs.at[mine], d_send, d_recv, partner)
    go(d_copy)
    wo_copy.wait()
    swap.wait_send()
    push(wo.at[:, pl.ds(0, HALF)], wbuf2.at[pl.ds(pl.multiple_of((1 - me.c) * ROWS, 64), ROWS)], swap_send, swap_recv,
         partner).wait_recv()
    push(lhs.at[theirs], lhs.at[theirs], d_send, d_recv, partner).wait_recv()

    def rows_of(j):
        return pl.ds(pl.multiple_of(j * 8, 8), 8)

    width = HALF // PARTS

    def cols_of(q):
        return pl.ds(q * width, width)

    b2 = [[push(p.at[rows_of(order[i]), cols_of(q)], rb2.at[i, q], b2_send.at[i, q], b2_recv.at[i, q], y_peer)
           for q in range(PARTS)] for i in range(4)]
    m2 = [[push(mb2.at[i, q], rm2.at[i, q], m2_send.at[i, q], m2_recv.at[i, q], mate) for q in range(PARTS)]
          for i in range(3)]
    f2 = [[push(mc2.at[i, q], rf2.at[q], f2_send.at[i, q], f2_recv.at[q], peer) for q in range(PARTS)]
          for i, peer in enumerate((far_end, far_inner))]
    for q in range(PARTS):
        at = q * width
        p[:, at:at + width] = jnp.dot(lhs[...], wbuf2[:, at:at + width], preferred_element_type=F32)
        for i in range(2):
            go(b2[i][q])
    for i in range(2, 4):
        for q in range(PARTS):
            go(b2[i][q])

    def y2_step(i, q):
        b2[i][q].wait_recv()
        mb2[i, q] = p[rows_of(order[4 + i]), q * width:(q + 1) * width] + rb2[i, q]
        if i < 2:
            if_end(lambda: go(m2[i][q], at_end))
        elif i == 2:
            go(m2[i][q])

    def m2_step(i, q):
        m2[i][q].wait_recv()
        mc2[i, q] = mb2[i, q] + rm2[i, q]
        go(f2[i][q], at_inner)

    def part(j, c, q):
        return out.at[rows_of(j), pl.ds(pl.multiple_of(c * HALF + q * width, LANES), width)]

    whole = Gather(me, lambda j, q: part(j, me.c, q), lambda j, q: part(j, 1 - me.c, q), sems[6:])

    def finish(q):
        m2[2][q].wait_recv()
        f2[0][q].wait_recv()
        total = (mb2[3, q] + rm2[2, q]) + rf2[q]
        out[rows_of(me.j), pl.ds(pl.multiple_of(me.c * HALF + q * width, LANES), width)] = total.astype(BF16)
        whole.start(q)

    for kind, i, q in read_steps(OUT_STEPS):
        if kind == 0:
            y2_step(i, q)
        elif kind == 1:
            if_inner(lambda: m2_step(i, q))
        else:
            finish(q)
    for q in range(PARTS):
        whole.from_z(q)
    for q in range(PARTS):
        whole.from_y(q)
    for q in range(PARTS):
        whole.from_core(q)
    for q in range(PARTS):
        whole.sent(q)
    for copy in started:
        copy.wait_send()

    @if_end
    def _():
        for copy in at_end:
            copy.wait_send()

    @if_inner
    def _():
        for copy in at_inner:
            copy.wait_send()


def write_kernel(pos, kn, vn, y_in, k_in, v_in, k, v, ko, vo, y, k_sem, v_sem, y_sem):
    y_copy = pltpu.make_async_copy(y_in, y, y_sem)
    y_copy.start()
    first = lax.axis_index('seq') * 64

    def out(i):
        bs = pl.ds(i * 16, 16)
        return [pltpu.make_async_copy(k.at[bs], ko.at[bs], k_sem.at[i]),
                pltpu.make_async_copy(v.at[bs], vo.at[bs], v_sem.at[i])]

    for i in range(4):
        for e in range(16):
            b = i * 16 + e
            at = lax.rem(i, 2) * 32 + i // 2 * 16 + e
            row = pos[b] - first
            here = jnp.logical_and(row >= 0, row < 64)
            rows = pl.ds(pl.multiple_of(jnp.clip(row, 0, 63) * 8, 8), 8)
            k[b, rows, :] = jnp.where(here, kn[at, 0:8], k[b, rows, :])
            v[b, rows, :] = jnp.where(here, vn[at, 0:8], v[b, rows, :])
        for copy in out(i):
            copy.start()
    for i in range(4):
        for copy in out(i):
            copy.wait()
    y_copy.wait()


def dma(*shape):
    return pltpu.SemaphoreType.DMA(shape) if shape else pltpu.SemaphoreType.DMA


def solution(mesh):
    cache_spec = P('rep', 'seq', None, None)
    in_specs = (P('rep', None), P(), P(), P(), P('seq', None), cache_spec, cache_spec, P('rep'))
    out_specs = (P('rep', None), cache_spec, cache_spec)
    shape = jax.ShapeDtypeStruct

    def step(x, wq, wk, wv, wo, k, v, pos):
        cache = (64, 512, LANES)
        rows = pltpu.VMEM((64, 16, LANES), BF16)
        piece = (32, 8, LANES)
        stat = pltpu.VMEM((2, 2, 8, LANES), F32)

        def pieces(n):
            return pltpu.VMEM((n,) + piece, F32)

        def sums(n):
            return pltpu.VMEM((n, PARTS, 8, HALF // PARTS), F32)

        held = [pltpu.with_memory_space_constraint(a, pltpu.HBM)
                for a in (pos, x, wq, wk, wv, wo, k.reshape(cache), v.reshape(cache))]
        y, k2, v2, kn, vn = pl.pallas_call(
            step_kernel,
            out_shape=[pltpu.VMEM((64, D), BF16), pltpu.VMEM(cache, BF16), pltpu.VMEM(cache, BF16), rows, rows],
            in_specs=[HBM] * 8,
            out_specs=[VMEM] * 5,
            scratch_shapes=[
                pltpu.VMEM((2, 8, 9, 32, LANES), BF16), pltpu.VMEM((64, D), BF16), pltpu.VMEM((D, 640), BF16),
                pltpu.VMEM((64 * PITCH, LANES), F32), pltpu.VMEM((8 * PITCH, LANES), F32),
                pltpu.VMEM((8, 64, 8, LANES), F32), pltpu.VMEM((2, 4, 8, LANES), F32),
                pieces(8), stat, pieces(8), stat, pieces(4), stat, pieces(4), stat, pieces(3), stat, pieces(2), stat,
                pltpu.VMEM(piece, F32), stat,
                pltpu.VMEM((256, LANES), F32), pltpu.VMEM((64, 896), BF16), pltpu.VMEM((896, HALF), BF16),
                pltpu.VMEM((64, HALF), F32), sums(4), sums(4), sums(3), sums(2), pltpu.VMEM((PARTS, 8, HALF // PARTS), F32),
                pltpu.SMEM((64,), jnp.int32), dma(), dma(), dma(CHUNKS, 3), dma(2, SLICES), dma(), dma(), dma(),
                dma(8, 2), dma(8, 2), dma(4, PARTS), dma(4, PARTS), dma(3, PARTS), dma(3, PARTS), dma(2, PARTS), dma(PARTS),
                dma(2), dma(2), dma(2), dma(2), dma(2), dma(2), dma(2, 2), dma(2),
                dma(), dma(), dma(4, PARTS), dma(4, PARTS), dma(3, PARTS), dma(3, PARTS), dma(2, PARTS), dma(PARTS),
            ] + gather_sems(2) + gather_sems(PARTS),
            cost_estimate=pl.CostEstimate(flops=10 ** 10, bytes_accessed=10 ** 7, transcendentals=0),
            compiler_params=pltpu.CompilerParams(
                collective_id=1, has_side_effects=True, vmem_limit_bytes=36 * 2 ** 20),
            name='attend_step',
        )(*held)
        _, _, ko, vo, y = pl.pallas_call(
            write_kernel,
            out_shape=[pltpu.VMEM(cache, BF16), pltpu.VMEM(cache, BF16), shape(cache, BF16), shape(cache, BF16),
                       shape((64, D), BF16)],
            in_specs=[SMEM] + [VMEM] * 5,
            out_specs=[VMEM, VMEM, HBM, HBM, HBM],
            input_output_aliases={4: 0, 5: 1},
            scratch_shapes=[dma(4), dma(4), dma()],
            cost_estimate=pl.CostEstimate(flops=10 ** 9, bytes_accessed=4 * 10 ** 7, transcendentals=0),
            compiler_params=pltpu.CompilerParams(vmem_limit_bytes=30 * 2 ** 20),
            name='write_caches',
        )(pos, kn, vn, y, k2, v2)
        return y, ko.reshape(k.shape), vo.reshape(v.shape)

    return jax.shard_map(step, mesh=mesh, in_specs=in_specs, out_specs=out_specs, check_vma=False)
```

```python
import functools

import jax
import jax.numpy as jnp
from jax import lax
from jax.experimental import pallas as pl
from jax.experimental.pallas import tpu as pltpu
from jax.sharding import PartitionSpec as P

MESH = pl.DeviceIdType.MESH
F32, BF16 = jnp.float32, jnp.bfloat16
VMEM = pl.BlockSpec(memory_space=pltpu.VMEM)
HBM = pl.BlockSpec(memory_space=pltpu.HBM)
SMEM = pl.BlockSpec(memory_space=pltpu.SMEM)
LOWEST = float(jnp.finfo(jnp.float32).min)
LANES = 128
D = 7168
HALF = D // 2
ROWS = 448
CHUNKS = 4
GROUP = 1
SLICES = 4
PARTS = 4
USED = slice(0, 7)
BATCH = 16
PITCH = 65
CHUNK = D // CHUNKS


Y_STEPS = ('y00y01y10y11y20y21', 'y02y03m00m01y12m10y13m11y22m02y23m03y30m12y31m13y32y33')
OUT_STEPS = ('y00y10y01y11y02m00y12m10y03m01y13m11y20m02', 'y21m12y22m03y23m13y30f00y31f01y32f02y33f03')


def read_steps(lines):
    return [('ymf'.index(line[n]), int(line[n + 1]), int(line[n + 2])) for line in lines
            for n in range(0, len(line), 3)]


class Place:
    def __init__(self):
        self.rep = lax.axis_index('rep')
        seq = lax.axis_index('seq')
        self.z = seq // 4
        self.y = lax.rem(seq // 2, 2)
        self.c = lax.rem(seq, 2)
        self.j = seq // 2

    def at(self, z, y, c):
        return (self.rep, (z * 2 + y) * 2 + c)

    def others(self):
        z = self.z
        low = 1 - z // 2
        return [low * 3, 1 + low, z + 1 - 2 * lax.rem(z, 2), z]

    def inner(self):
        return jnp.logical_and(self.z >= 1, self.z <= 2)

    def greet(self):
        barrier = pltpu.get_barrier_semaphore()
        peers = [self.at(self.z, self.y, 1 - self.c), self.at(self.z, 1 - self.y, self.c)]
        peers += [self.at(zz, self.y, self.c) for zz in self.others()[:3]]
        for peer in peers:
            pl.semaphore_signal(barrier, inc=1, device_id=peer, device_id_type=MESH)
        pl.semaphore_wait(barrier, len(peers))


def push(src, dst, send, recv, device):
    copy = pltpu.make_async_remote_copy(
        src_ref=src, dst_ref=dst, send_sem=send, recv_sem=recv, device_id=device, device_id_type=MESH)
    return copy


class Gather:
    def __init__(self, me, region, other, sems):
        self.me, self.region, self.other = me, region, other
        self.z_send, self.z_recv, self.y_send, self.y_recv, self.c_send, self.c_recv = sems
        self.zs = me.others()

    def go(self, copy):
        copy.start()

    def along_z(self, h, i, j, arrival=False):
        src = self.region(j, h)
        slot = i if arrival or i == 2 else lax.rem((self.me.z + 1) // 2, 2)
        return push(src, src, self.z_send.at[h, i], self.z_recv.at[h, slot],
                    self.me.at(self.zs[i], self.me.y, self.me.c))

    def across_y(self, h, i, j):
        src = self.region(j, h)
        return push(src, src, self.y_send.at[h, i], self.y_recv.at[h, i],
                    self.me.at(self.me.z, 1 - self.me.y, self.me.c))

    def to_core(self, h, i, src):
        return push(src, src, self.c_send.at[h, i], self.c_recv.at[h, i],
                    self.me.at(self.me.z, self.me.y, 1 - self.me.c))

    def start(self, h):
        for i in range(3):
            self.go(self.along_z(h, i, self.me.j))
        self.go(self.across_y(h, 3, self.me.j))
        self.go(self.to_core(h, 3, self.region(self.me.j, h)))

    def near(self, i):
        return self.zs[i] * 2 + self.me.y

    def far(self, i):
        return self.zs[i] * 2 + 1 - self.me.y

    def from_z(self, h):
        for i in (2, 1, 0):
            self.along_z(h, i, self.near(i), arrival=True).wait_recv()
            self.go(self.across_y(h, i, self.near(i)))
            self.go(self.to_core(h, i, self.region(self.near(i), h)))

    def from_y(self, h):
        for i in (3, 2, 1, 0):
            self.across_y(h, i, self.far(i)).wait_recv()
            self.go(self.to_core(h, 4 + i, self.region(self.far(i), h)))

    def from_core(self, h):
        for i in (3, 2, 1, 0):
            self.to_core(h, i, self.other(self.near(i), h)).wait_recv()
            self.to_core(h, 4 + i, self.other(self.far(i), h)).wait_recv()

    def sent(self, h):
        for i in range(3):
            self.along_z(h, i, self.me.j).wait_send()
        for i in range(4):
            self.across_y(h, i, self.near(i)).wait_send()
            self.to_core(h, i, self.region(self.near(i), h)).wait_send()
            self.to_core(h, 4 + i, self.region(self.far(i), h)).wait_send()


def gather_sems(parts):
    return [pltpu.SemaphoreType.DMA((parts, n)) for n in (3, 3, 4, 4, 8, 8)]


TILES = ((0, 5), (5, 4))


def step_kernel(pos_in, x_in, wq, wk, wv, wo, k_in, v_in, out, k, v, kn, vn,
                g, x, wbuf, qs, vs, o, stats, ra, sa, ma, sma, rb, sb, mb, smb, rm, sm, mc, smc, rf, sf, fin, lhs,
                wbuf2, p, rb2, mb2, rm2, mc2, rf2,
                pos, pos_sem, x_sem, w_sem, kv_sem, wo_sem, swap_send, swap_recv, a_send, a_recv, b_send, b_recv, m_send, m_recv,
                f_send, f_recv, as_send, as_recv, bs_send, bs_recv, ms_send, ms_recv, fs_send, fs_recv,
                d_send, d_recv, b2_send, b2_recv, m2_send, m2_recv, f2_send, f2_recv, *sems):
    me = Place()
    zs = me.others()
    partner = me.at(me.z, me.y, 1 - me.c)
    y_peer = me.at(me.z, 1 - me.y, me.c)
    far_end, far_inner, mate = [me.at(zs[i], me.y, me.c) for i in range(3)]
    mine = pl.ds(pl.multiple_of(me.c * 32, 32), 32)
    theirs = pl.ds(pl.multiple_of((1 - me.c) * 32, 32), 32)
    started, at_end, at_inner = [], [], []

    def go(copy, kept=started):
        copy.start()
        kept.append(copy)

    def if_inner(f):
        pl.when(me.inner())(f)

    def if_end(f):
        pl.when(jnp.logical_not(me.inner()))(f)

    x_copy = pltpu.make_async_copy(x_in, x, x_sem)
    pos_copy = pltpu.make_async_copy(pos_in, pos, pos_sem)
    pos_copy.start()
    cache = []
    for i in range(SLICES):
        bs = slice(i * 64 // SLICES, (i + 1) * 64 // SLICES)
        cache += [pltpu.make_async_copy(k_in.at[bs], k.at[bs], kv_sem.at[0, i]),
                  pltpu.make_async_copy(v_in.at[bs], v.at[bs], kv_sem.at[1, i])]

    def weights(c, i):
        rows = pl.ds(i * CHUNK, CHUNK)
        if c == 0:
            parts = [(wq, me.j * 896, 640)]
        else:
            parts = [(wq, me.j * 896 + 640, 256), (wk, me.j * LANES, LANES), (wv, me.j * LANES, LANES)]
        at, copies = 0, []
        for n, (w, col, width) in enumerate(parts):
            copies.append(pltpu.make_async_copy(w.at[rows, pl.ds(pl.multiple_of(col, LANES), width)],
                                                wbuf.at[rows, at:at + width], w_sem.at[i, n]))
            at += width
        return copies

    for c in range(2):
        @pl.when(me.c == c)
        def _(c=c):
            for i in range(CHUNKS):
                for copy in weights(c, i):
                    copy.start()
                if i == 0:
                    x_copy.start()

    me.greet()
    x_copy.wait()
    for c in range(2):
        @pl.when(me.c == c)
        def _(c=c):
            lo, n = TILES[c]
            acc = jnp.zeros((64, n * LANES), F32)
            rows = GROUP * CHUNK
            for i in range(CHUNKS // GROUP):
                for u in range(GROUP):
                    for copy in weights(c, i * GROUP + u):
                        copy.wait()
                acc += jnp.dot(x[:, i * rows:(i + 1) * rows], wbuf[i * rows:(i + 1) * rows, :n * LANES],
                               preferred_element_type=F32)
            for h in range(2):
                for q in range(2):
                    for t in range(n):
                        g[h, me.j, lo + t, q * 16:q * 16 + 16] = acc[
                            q * 32 + h * 16:q * 32 + h * 16 + 16, t * LANES:(t + 1) * LANES].astype(BF16)

    wo_copy = pltpu.make_async_copy(wo.at[:, pl.ds(pl.multiple_of(me.c * HALF, LANES), HALF)],
                                    wbuf2.at[pl.ds(pl.multiple_of(me.c * ROWS, 64), ROWS)], wo_sem)
    swap = push(wo.at[:, pl.ds(pl.multiple_of((1 - me.c) * HALF, LANES), HALF)],
                wbuf2.at[pl.ds(pl.multiple_of(me.c * ROWS, 64), ROWS)], swap_send, swap_recv, partner)

    def begin_caches():
        for copy in cache:
            copy.start()
        wo_copy.start()
        swap.start()

    def inputs(f):
        for c in range(2):
            @pl.when(me.c == c)
            def _(c=c):
                lo, n = TILES[c]
                lo2, n2 = TILES[1 - c]
                f(Gather(me, lambda j, h: g.at[h, j, lo:lo + n], lambda j, h: g.at[h, j, lo2:lo2 + n2], sems[:6]))

    def gather_first(w):
        w.start(0)
        w.start(1)

    def gather_relay(w):
        w.from_z(0)
        w.from_z(1)
        w.from_y(0)
        w.from_core(0)

    def gather_last(w):
        w.from_core(1)
        w.sent(0)
        w.sent(1)

    inputs(gather_first)
    begin_caches()
    inputs(gather_relay)
    for copy in cache:
        copy.wait()
    pos_copy.wait()

    first = lax.axis_index('seq') * 64
    s_of = lax.broadcasted_iota(jnp.int32, (8, LANES), 1) // 8
    lane = lax.broadcasted_iota(jnp.int32, (8, 512), 1)
    is_head = [lax.rem(lane, 8) == n for n in range(8)]
    at_of = lane // 8
    row_of = lax.broadcasted_iota(jnp.int32, (512, LANES), 0) // 8

    def spread(h):
        def head(j, _):
            for t in range(8):
                qs[pl.ds((j * 8 + t) * PITCH + h * 32, 32), :] = g[h, j, t].astype(F32)
            vs[pl.ds(j * PITCH + h * 32, 32), :] = g[h, j, 8].astype(F32)
            return 0

        lax.fori_loop(0, 8, head, 0)

        def news(e, _):
            at = h * 32 + e
            for to, new in ((kn, qs[pl.ds(7 * PITCH + at, 8, stride=8 * PITCH), :]),
                            (vn, vs[pl.ds(at, 8, stride=PITCH), :])):
                to[at] = jnp.concatenate([new, new], axis=0).astype(BF16)
            return 0

        lax.fori_loop(0, 32, news, 0, unroll=8)

    def with_new(ref, b, new, limit):
        return jnp.where(row_of == limit, jnp.concatenate([new] * 32, axis=0), ref[b])

    def scores(b, at):
        q = qs[pl.ds(at, 64, stride=PITCH), :].astype(BF16)
        limit = pos[b] - first
        s = lax.dot_general(q, with_new(k, b, kn[at], limit), (((1,), (1,)), ((), ())), preferred_element_type=F32)
        t = s[0:8]
        for hd in range(1, 8):
            t = jnp.where(is_head[hd], s[hd * 8:hd * 8 + 8], t)
        valid = at_of <= limit
        return jnp.where(valid, t * (LANES ** -0.5), LOWEST), valid

    def quarters(a):
        return [a[:, n * LANES:(n + 1) * LANES] for n in range(4)]

    def soften(batch):
        m = []
        for t, _ in batch:
            q = quarters(t)
            m.append(jnp.maximum(jnp.maximum(q[0], q[1]), jnp.maximum(q[2], q[3])))
        for shift in (8, 16, 32, 64):
            turned = [pltpu.roll(a, shift, 1) for a in m]
            m = [jnp.maximum(a, b) for a, b in zip(m, turned)]
        e = [jnp.where(valid, jnp.exp(t - jnp.concatenate([a] * 4, axis=1)), 0.0) for (t, valid), a in zip(batch, m)]
        l = []
        for w in e:
            q = quarters(w)
            l.append((q[0] + q[1]) + (q[2] + q[3]))
        for shift in (8, 16, 32, 64):
            turned = [pltpu.roll(a, shift, 1) for a in l]
            l = [a + b for a, b in zip(l, turned)]
        return m, l, e

    def values(b, at, e):
        w = jnp.concatenate([jnp.where(is_head[hd], e, 0.0) for hd in range(8)], axis=0).astype(BF16)
        ob = jnp.dot(w, with_new(v, b, vn[at], pos[b] - first), preferred_element_type=F32)
        for hd in range(8):
            o[hd, b] = ob[hd * 8:hd * 8 + 8]

    def attend(h, q):
        places = [(q * 32 + h * 16 + e, h * 32 + q * 16 + e) for e in range(16)]
        ahead = [scores(*place) for place in places[:BATCH]]
        ms = ls = jnp.zeros((8, LANES), F32)
        for i in range(16 // BATCH):
            batch, ahead = ahead, []
            if i + 1 < 16 // BATCH:
                ahead = [scores(*place) for place in places[(i + 1) * BATCH:(i + 2) * BATCH]]
            m, l, w = soften(batch)
            for e in range(BATCH):
                bb = i * BATCH + e
                values(*places[bb], w[e])
                here = s_of == bb
                ms, ls = jnp.where(here, m[e], ms), jnp.where(here, l[e], ls)
        stats[0, q * 2 + h] = ms
        stats[1, q * 2 + h] = ls

    order = [zs[i] * 2 + 1 - me.y for i in range(4)] + [zs[i] * 2 + me.y for i in range(4)]
    a_stat = [push(stats.at[:, (1 - me.c) * 2 + h], sa.at[:, h], as_send.at[h], as_recv.at[h], partner)
              for h in range(2)]
    a = [[push(o.at[order[i], pl.ds((1 - me.c) * 32 + h * 16, 16), USED], ra.at[i, h * 16:h * 16 + 16, USED],
               a_send.at[i, h], a_recv.at[i, h], partner) for h in range(2)] for i in range(8)]

    def exchange(h):
        go(a_stat[h])
        for i in range(8):
            go(a[i][h])

    def weights_of(m_list, l_list):
        top = m_list[0]
        for m in m_list[1:]:
            top = jnp.maximum(top, m)
        scale = [jnp.exp(m - top) for m in m_list]
        total = scale[0] * l_list[0]
        for f, l in zip(scale[1:], l_list[1:]):
            total = total + f * l
        return top, total, scale

    def blend(stat_refs, h, out_ref=None, divide=False):
        top, total, scale = weights_of([r(0, h) for r in stat_refs], [r(1, h) for r in stat_refs])
        if out_ref is not None:
            out_ref[0, h], out_ref[1, h] = top, total
        return [f / total for f in scale] if divide else scale

    def merge(head, q, factors, sources, store):
        turned = [pltpu.roll(f, lax.rem(LANES - head, LANES), 1) for f in factors]
        for bb in range(8):
            total = None
            lane0 = (q % 2 * 8 + bb) * 8
            for f, source in zip(turned, sources):
                term = source(q * 8 + bb) * jnp.broadcast_to(f[:, lane0:lane0 + 1], (8, LANES))
                total = term if total is None else total + term
            store(q * 8 + bb, total)

    def of(ref, i):
        return lambda b: ref[i, b]

    def into(ref, i):
        def store(b, value):
            ref[i, b] = value
        return store

    def unit(ref, i, q):
        return ref.at[i, q * 8:q * 8 + 8, USED]

    def stat(ref):
        return lambda s, h: ref[s, h]

    b_stat = [push(sma.at[:, h], sb.at[:, h], bs_send.at[h], bs_recv.at[h], y_peer) for h in range(2)]
    b = [[push(unit(ma, i, q), unit(rb, i, q), b_send.at[i, q], b_recv.at[i, q], y_peer) for q in range(PARTS)]
         for i in range(4)]
    by_core = [None, None]

    def core_step(h, some):
        if by_core[h] is None:
            a_stat[h].wait_recv()
            by_core[h] = blend([lambda s, h: stats[s, me.c * 2 + h], stat(sa)], h, sma)
            go(b_stat[h])
        for i in some:
            a[i][h].wait_recv()
        for i in some:
            for q in (2 * h, 2 * h + 1):
                merge(order[i], q, by_core[h], [lambda bb, i=i: o[order[i], me.c * 32 + bb], of(ra, i)], into(ma, i))
        for i in some:
            if i < 4:
                go(b[i][2 * h])
                go(b[i][2 * h + 1])

    spread(0)
    attend(0, 1 - me.c)
    inputs(lambda w: w.from_y(1))
    exchange(0)
    attend(0, me.c)
    core_step(0, range(3))
    inputs(gather_last)
    spread(1)
    attend(1, 1 - me.c)
    exchange(1)
    attend(1, me.c)
    core_step(1, range(3))
    core_step(0, range(4, 7))

    m_stat = [push(smb.at[:, h], sm.at[:, h], ms_send.at[h], ms_recv.at[h], mate) for h in range(2)]
    m = [[push(unit(mb, i, q), unit(rm, i, q), m_send.at[i, q], m_recv.at[i, q], mate) for q in range(PARTS)]
         for i in range(3)]
    f = [[push(unit(mc, i, q), rf.at[q * 8:q * 8 + 8, USED], f_send.at[i, q], f_recv.at[q], peer)
          for q in range(PARTS)] for i, peer in enumerate((far_end, far_inner))]
    f_stat = [[push(smc.at[:, h], sf.at[:, h], fs_send.at[i, h], fs_recv.at[h], peer) for h in range(2)]
              for i, peer in enumerate((far_end, far_inner))]
    by_y = [None, None]

    def y_step(i, q):
        h = q // 2
        if by_y[h] is None:
            b_stat[h].wait_recv()
            by_y[h] = blend([stat(sma), stat(sb)], h, smb)
            go(m_stat[h])
        b[i][q].wait_recv()
        merge(order[4 + i], q, by_y[h], [of(ma, 4 + i), of(rb, i)], into(mb, i))
        if i < 2:
            if_end(lambda: go(m[i][q], at_end))
        elif i == 2:
            go(m[i][q])

    def m_step(i, q):
        h = q // 2
        opens = i == 0 and q % 2 == 0
        if opens:
            m_stat[h].wait_recv()
        factors = blend([stat(smb), stat(sm)], h, smc if opens else None)
        if opens:
            for copy in f_stat:
                go(copy[h], at_inner)
        m[i][q].wait_recv()
        merge(order[4 + i], q, factors, [of(mb, i), of(rm, i)], into(mc, i))
        go(f[i][q], at_inner)

    for line in Y_STEPS:
        for inner, i, q in read_steps((line,)):
            if not inner:
                y_step(i, q)
            else:
                if_inner(lambda: m_step(i, q))
        if line is Y_STEPS[0]:
            core_step(1, range(3, 8))
            core_step(0, (3, 7))

    for q in range(PARTS):
        h = q // 2
        if q % 2 == 0:
            if_end(m_stat[h].wait_recv)
            f_stat[0][h].wait_recv()
            by_z = blend([stat(smb), stat(sm), stat(sf)], h, divide=True)
        m[2][q].wait_recv()
        f[0][q].wait_recv()

        def final(b, value):
            fin[pl.ds(b * 8, 8), :] = value

        merge(order[7], q, by_z, [of(mb, 3), of(rm, 2), lambda b: rf[b]], final)
    for t in range(7):
        lhs[mine, t * LANES:(t + 1) * LANES] = fin[pl.ds(t, 32, stride=8), :].astype(BF16)
    d_copy = push(lhs.at[mine], lhs.at[mine], d_send, d_recv, partner)
    go(d_copy)
    wo_copy.wait()
    swap.wait_send()
    push(wo.at[:, pl.ds(0, HALF)], wbuf2.at[pl.ds(pl.multiple_of((1 - me.c) * ROWS, 64), ROWS)], swap_send, swap_recv,
         partner).wait_recv()
    push(lhs.at[theirs], lhs.at[theirs], d_send, d_recv, partner).wait_recv()

    def rows_of(j):
        return pl.ds(pl.multiple_of(j * 8, 8), 8)

    width = HALF // PARTS

    def cols_of(q):
        return pl.ds(q * width, width)

    b2 = [[push(p.at[rows_of(order[i]), cols_of(q)], rb2.at[i, q], b2_send.at[i, q], b2_recv.at[i, q], y_peer)
           for q in range(PARTS)] for i in range(4)]
    m2 = [[push(mb2.at[i, q], rm2.at[i, q], m2_send.at[i, q], m2_recv.at[i, q], mate) for q in range(PARTS)]
          for i in range(3)]
    f2 = [[push(mc2.at[i, q], rf2.at[q], f2_send.at[i, q], f2_recv.at[q], peer) for q in range(PARTS)]
          for i, peer in enumerate((far_end, far_inner))]
    for q in range(PARTS):
        at = q * width
        p[:, at:at + width] = jnp.dot(lhs[...], wbuf2[:, at:at + width], preferred_element_type=F32)
        for i in range(2):
            go(b2[i][q])
    for i in range(2, 4):
        for q in range(PARTS):
            go(b2[i][q])

    def y2_step(i, q):
        b2[i][q].wait_recv()
        mb2[i, q] = p[rows_of(order[4 + i]), q * width:(q + 1) * width] + rb2[i, q]
        if i < 2:
            if_end(lambda: go(m2[i][q], at_end))
        elif i == 2:
            go(m2[i][q])

    def m2_step(i, q):
        m2[i][q].wait_recv()
        mc2[i, q] = mb2[i, q] + rm2[i, q]
        go(f2[i][q], at_inner)

    def part(j, c, q):
        return out.at[rows_of(j), pl.ds(pl.multiple_of(c * HALF + q * width, LANES), width)]

    whole = Gather(me, lambda j, q: part(j, me.c, q), lambda j, q: part(j, 1 - me.c, q), sems[6:])

    def finish(q):
        m2[2][q].wait_recv()
        f2[0][q].wait_recv()
        total = (mb2[3, q] + rm2[2, q]) + rf2[q]
        out[rows_of(me.j), pl.ds(pl.multiple_of(me.c * HALF + q * width, LANES), width)] = total.astype(BF16)
        whole.start(q)

    for kind, i, q in read_steps(OUT_STEPS):
        if kind == 0:
            y2_step(i, q)
        elif kind == 1:
            if_inner(lambda: m2_step(i, q))
        else:
            finish(q)
    for q in range(PARTS):
        whole.from_z(q)
    for q in range(PARTS):
        whole.from_y(q)
    for q in range(PARTS):
        whole.from_core(q)
    for q in range(PARTS):
        whole.sent(q)
    for copy in started:
        copy.wait_send()

    @if_end
    def _():
        for copy in at_end:
            copy.wait_send()

    @if_inner
    def _():
        for copy in at_inner:
            copy.wait_send()


def write_kernel(pos, kn, vn, y_in, k_in, v_in, k, v, ko, vo, y, k_sem, v_sem, y_sem):
    y_copy = pltpu.make_async_copy(y_in, y, y_sem)
    y_copy.start()
    first = lax.axis_index('seq') * 64

    def out(i):
        bs = pl.ds(i * 16, 16)
        return [pltpu.make_async_copy(k.at[bs], ko.at[bs], k_sem.at[i]),
                pltpu.make_async_copy(v.at[bs], vo.at[bs], v_sem.at[i])]

    for i in range(4):
        for e in range(16):
            b = i * 16 + e
            at = lax.rem(i, 2) * 32 + i // 2 * 16 + e
            row = pos[b] - first
            here = jnp.logical_and(row >= 0, row < 64)
            rows = pl.ds(pl.multiple_of(jnp.clip(row, 0, 63) * 8, 8), 8)
            k[b, rows, :] = jnp.where(here, kn[at, 0:8], k[b, rows, :])
            v[b, rows, :] = jnp.where(here, vn[at, 0:8], v[b, rows, :])
        for copy in out(i):
            copy.start()
    for i in range(4):
        for copy in out(i):
            copy.wait()
    y_copy.wait()


def dma(*shape):
    return pltpu.SemaphoreType.DMA(shape) if shape else pltpu.SemaphoreType.DMA


def solution(mesh):
    cache_spec = P('rep', 'seq', None, None)
    in_specs = (P('rep', None), P(), P(), P(), P('seq', None), cache_spec, cache_spec, P('rep'))
    out_specs = (P('rep', None), cache_spec, cache_spec)
    shape = jax.ShapeDtypeStruct

    def step(x, wq, wk, wv, wo, k, v, pos):
        cache = (64, 512, LANES)
        rows = pltpu.VMEM((64, 16, LANES), BF16)
        piece = (32, 8, LANES)
        stat = pltpu.VMEM((2, 2, 8, LANES), F32)

        def pieces(n):
            return pltpu.VMEM((n,) + piece, F32)

        def sums(n):
            return pltpu.VMEM((n, PARTS, 8, HALF // PARTS), F32)

        held = [pltpu.with_memory_space_constraint(a, pltpu.HBM)
                for a in (pos, x, wq, wk, wv, wo, k.reshape(cache), v.reshape(cache))]
        y, k2, v2, kn, vn = pl.pallas_call(
            step_kernel,
            out_shape=[pltpu.VMEM((64, D), BF16), pltpu.VMEM(cache, BF16), pltpu.VMEM(cache, BF16), rows, rows],
            in_specs=[HBM] * 8,
            out_specs=[VMEM] * 5,
            scratch_shapes=[
                pltpu.VMEM((2, 8, 9, 32, LANES), BF16), pltpu.VMEM((64, D), BF16), pltpu.VMEM((D, 640), BF16),
                pltpu.VMEM((64 * PITCH, LANES), F32), pltpu.VMEM((8 * PITCH, LANES), F32),
                pltpu.VMEM((8, 64, 8, LANES), F32), pltpu.VMEM((2, 4, 8, LANES), F32),
                pieces(8), stat, pieces(8), stat, pieces(4), stat, pieces(4), stat, pieces(3), stat, pieces(2), stat,
                pltpu.VMEM(piece, F32), stat,
                pltpu.VMEM((256, LANES), F32), pltpu.VMEM((64, 896), BF16), pltpu.VMEM((896, HALF), BF16),
                pltpu.VMEM((64, HALF), F32), sums(4), sums(4), sums(3), sums(2), pltpu.VMEM((PARTS, 8, HALF // PARTS), F32),
                pltpu.SMEM((64,), jnp.int32), dma(), dma(), dma(CHUNKS, 3), dma(2, SLICES), dma(), dma(), dma(),
                dma(8, 2), dma(8, 2), dma(4, PARTS), dma(4, PARTS), dma(3, PARTS), dma(3, PARTS), dma(2, PARTS), dma(PARTS),
                dma(2), dma(2), dma(2), dma(2), dma(2), dma(2), dma(2, 2), dma(2),
                dma(), dma(), dma(4, PARTS), dma(4, PARTS), dma(3, PARTS), dma(3, PARTS), dma(2, PARTS), dma(PARTS),
            ] + gather_sems(2) + gather_sems(PARTS),
            cost_estimate=pl.CostEstimate(flops=10 ** 10, bytes_accessed=10 ** 7, transcendentals=0),
            compiler_params=pltpu.CompilerParams(
                collective_id=1, has_side_effects=True, vmem_limit_bytes=36 * 2 ** 20),
            name='attend_step',
        )(*held)
        _, _, ko, vo, y = pl.pallas_call(
            write_kernel,
            out_shape=[pltpu.VMEM(cache, BF16), pltpu.VMEM(cache, BF16), shape(cache, BF16), shape(cache, BF16),
                       shape((64, D), BF16)],
            in_specs=[SMEM] + [VMEM] * 5,
            out_specs=[VMEM, VMEM, HBM, HBM, HBM],
            input_output_aliases={4: 0, 5: 1},
            scratch_shapes=[dma(4), dma(4), dma()],
            cost_estimate=pl.CostEstimate(flops=10 ** 9, bytes_accessed=4 * 10 ** 7, transcendentals=0),
            compiler_params=pltpu.CompilerParams(vmem_limit_bytes=30 * 2 ** 20),
            name='write_caches',
        )(pos, kn, vn, y, k2, v2)
        return y, ko.reshape(k.shape), vo.reshape(v.shape)

    return jax.shard_map(step, mesh=mesh, in_specs=in_specs, out_specs=out_specs, check_vma=False)
```
